8 devices in a mesh: lev: 1 (over z), w: 8 (over y, x, core).
Axes of the slice: x: 2, y: 2, z: 1, core: 2. Of those that a mesh axis runs over, the one named last changes fastest.
Arguments:
- coef: float32 [512, 2, 32, 512], P('w', None, 'lev')
- legendre: float32 [512, 512, 768], replicated
- gauss_weight: float32 [768], replicated
Outputs:
- output 1: float32 [32, 768, 1024], P('lev', 'w')
- output 2: float32 [512, 2, 32, 512], P('w', None, 'lev')
All inputs are finite; a program needn't handle non-finite values.
Results may differ from the reference program's by a relative error of at most 0.001.
Values sent between devices are 32-bit elements.
A program may use at most 3.25 GiB of HBM per device.

```python
import jax
import jax.numpy as jnp
from jax import lax

WAVE_NUM = 512
LAT_ROWS = 768
LEVELS = 32


def setup_inputs(seed: int = 0, part: int = 0) -> dict:
    base_key = jax.random.key(seed)
    key_coef = jax.random.fold_in(jax.random.fold_in(base_key, 1), part)
    key_leg = jax.random.fold_in(base_key, 2)
    key_wt = jax.random.fold_in(base_key, 3)
    wave_idx = jnp.arange(WAVE_NUM)
    row_m = wave_idx[:, None].astype(jnp.float32)
    col_l = wave_idx[None, :].astype(jnp.float32)
    live_mask = wave_idx[None, :] >= wave_idx[:, None]
    amplitude = jnp.sqrt(WAVE_NUM / ((WAVE_NUM - row_m) * (1.0 + (col_l - row_m) / WAVE_NUM)))
    coef_mask = jnp.stack([live_mask, live_mask & (wave_idx[:, None] > 0)], axis=1)[:, :, None, :]
    draw_coef = jax.random.normal(key_coef, (WAVE_NUM, 2, LEVELS, WAVE_NUM), jnp.float32)
    coef = jnp.where(coef_mask, draw_coef * amplitude[:, None, None, :], 0.0)
    draw_leg = jax.random.normal(key_leg, (WAVE_NUM, WAVE_NUM, LAT_ROWS), jnp.float32)
    legendre = jnp.where(live_mask[:, :, None], draw_leg, 0.0)
    gauss_weight = jax.random.uniform(key_wt, (LAT_ROWS,), jnp.float32, 0.5, 1.5) / LAT_ROWS
    return {'coef': coef, 'legendre': legendre, 'gauss_weight': gauss_weight}


def reference(coef, legendre, gauss_weight):
    lon_pts = 2 * WAVE_NUM
    splits = 8
    lat_blk = LAT_ROWS // splits

    def lat_step(spec_acc, blk_idx):
        lat_start = blk_idx * lat_blk
        leg_blk = lax.dynamic_slice_in_dim(legendre, lat_start, lat_blk, axis=2).astype(jnp.float32)
        wt_blk = lax.dynamic_slice_in_dim(gauss_weight, lat_start, lat_blk, axis=0)
        fourier = jnp.einsum('mrkl,mlj->mrkj', coef.astype(jnp.float32), leg_blk)
        spec = lax.complex(fourier[:, 0], fourier[:, 1])
        grid_blk = jnp.fft.irfft(spec, n=lon_pts, axis=0)
        square_hat = jnp.fft.rfft(grid_blk * grid_blk, axis=0)[:WAVE_NUM] * wt_blk[None, None, :]
        re_im = jnp.stack([jnp.real(square_hat), jnp.imag(square_hat)], axis=1)
        spec_acc = spec_acc + jnp.einsum('mrkj,mlj->mrkl', re_im, leg_blk)
        return spec_acc, jnp.transpose(grid_blk, (1, 2, 0))

    spec_out, grid_parts = lax.scan(lat_step, jnp.zeros(coef.shape, jnp.float32), jnp.arange(splits))
    grid = jnp.transpose(grid_parts, (1, 0, 2, 3)).reshape(LEVELS, LAT_ROWS, lon_pts)
    return grid, spec_out
```

```python
import functools

import jax
import jax.numpy as jnp
import numpy as np
from jax import lax
from jax.experimental import pallas as pl
from jax.experimental.pallas import tpu as pltpu
from jax.sharding import PartitionSpec as P

DEVS = 8
WAVES = 512
OWN = WAVES // DEVS
LATS = 768
LAT = LATS // DEVS
LEVS = 32
LONS = 1024
HALF = LONS // 2
KK = 8
QQ = 4
LANES = QQ * LAT
CHUNK = 8
NB = 3
ROWS = 2 * KK
BF = jnp.bfloat16
F32 = jnp.float32


def split(x):
    hi = x.astype(BF)
    return hi, (x - hi.astype(F32)).astype(BF)


def dot3(a_hi, a_lo, b_hi, b_lo, dims):
    mm = functools.partial(lax.dot_general, dimension_numbers=(dims, ((), ())), preferred_element_type=F32)
    return mm(a_hi, b_hi) + (mm(a_hi, b_lo) + mm(a_lo, b_hi))


def barrier_all(me):
    sem = pltpu.get_barrier_semaphore()
    for o in range(1, DEVS):
        pl.semaphore_signal(sem, inc=1, device_id={'w': lax.rem(me + o, DEVS)}, device_id_type=pl.DeviceIdType.MESH)
    pl.semaphore_wait(sem, DEVS - 1)


def own_wave(t):
    return 2 * lax.rem(t, OWN // 2) + lax.div(t, OWN // 2)


def inverse_legendre(coef, leg, recv, cbuf, lbuf, stage, csem, lsem, ssem, rsem):
    me = lax.axis_index('w')
    barrier_all(me)

    def fetches(t):
        slot = lax.rem(t, NB)
        m = own_wave(t)
        return (pltpu.make_async_copy(coef.at[m], cbuf.at[slot], csem.at[slot]), pltpu.make_async_copy(leg.at[me * OWN + m], lbuf.at[slot], lsem.at[slot]))

    def sends(c):
        slot = lax.rem(c, 2)
        row = lax.div(c, 4) * (WAVES // 2) + me * (OWN // 2) + lax.rem(c, 4) * CHUNK
        row = pl.multiple_of(row, CHUNK)
        out = []
        for o in range(DEVS):
            dst = lax.rem(me + o, DEVS)
            src_ref, dst_ref = stage.at[slot, dst], recv.at[:, pl.ds(row, CHUNK), :]
            if o == 0:
                out.append(pltpu.make_async_copy(src_ref, dst_ref, ssem.at[slot, 0]))
            else:
                out.append(pltpu.make_async_remote_copy(src_ref=src_ref, dst_ref=dst_ref, send_sem=ssem.at[slot, o], recv_sem=rsem.at[lax.div(c, 4), o], device_id={'w': dst}, device_id_type=pl.DeviceIdType.MESH))
        return out

    def wait_sends(c):
        for o, copy in enumerate(sends(c)):
            if o == 0:
                copy.wait()
            else:
                copy.wait_send()

    for t in range(NB):
        for copy in fetches(t):
            copy.start()

    @pl.loop(0, OWN // CHUNK)
    def _(c):
        slot = lax.rem(c, 2)

        @pl.when(c >= 2)
        def _():
            wait_sends(c - 2)

        @pl.loop(0, CHUNK)
        def _(i):
            t = c * CHUNK + i
            for copy in fetches(t):
                copy.wait()
            buf = lax.rem(t, NB)
            c_hi, c_lo = split(cbuf[buf].reshape(2 * LEVS, WAVES))
            l_hi, l_lo = split(lbuf[buf])
            f = dot3(c_hi, c_lo, l_hi, l_lo, ((1,), (0,)))

            @pl.when(t + NB < OWN)
            def _():
                for copy in fetches(t + NB):
                    copy.start()

            for d in range(DEVS):
                cols = f[:, d * LAT:(d + 1) * LAT]
                for r in range(2):
                    row = r * LEVS
                    packed = jnp.concatenate([cols[row + q * KK:row + (q + 1) * KK] for q in range(QQ)], axis=1)
                    for h in range(KK):
                        stage[slot, d, r * KK + h, pl.ds(i, 1), :] = packed[h:h + 1]

        for copy in sends(c):
            copy.start()

    wait_sends(OWN // CHUNK - 2)
    wait_sends(OWN // CHUNK - 1)
    for o in range(1, DEVS):
        src = lax.rem(me - o + DEVS, DEVS)
        for par in range(2):
            part = recv.at[:, pl.ds(pl.multiple_of(par * (WAVES // 2) + src * (OWN // 2), OWN // 2), OWN // 2), :]
            pltpu.make_async_copy(part, part, rsem.at[par, o]).wait()


def longitudes(f_in, dft, dft_t, weight, grid_out, recv, fbuf, gbuf, stage, fsem, gsem, ssem, rsem):
    me = lax.axis_index('w')
    barrier_all(me)

    def fetches(kk):
        slot = lax.rem(kk, 2)
        return [pltpu.make_async_copy(f_in.at[r * KK + kk], fbuf.at[slot, r], fsem.at[slot, r]) for r in range(2)]

    def stores(kk):
        slot = lax.rem(kk, 2)
        return [pltpu.make_async_copy(gbuf.at[slot, pl.ds(q * LAT, LAT)], grid_out.at[q * KK + kk], gsem.at[slot, q]) for q in range(QQ)]

    def sends(kk):
        slot = lax.rem(kk, 2)
        out = []
        for o in range(DEVS):
            dst = lax.rem(me + o, DEVS)
            src_ref = stage.at[slot, :, :, pl.ds(pl.multiple_of(dst * (OWN // 2), OWN // 2), OWN // 2), :]
            dst_ref = recv.at[me, :, :, kk]
            if o == 0:
                out.append(pltpu.make_async_copy(src_ref, dst_ref, ssem.at[slot, 0]))
            else:
                out.append(pltpu.make_async_remote_copy(src_ref=src_ref, dst_ref=dst_ref, send_sem=ssem.at[slot, o], recv_sem=rsem.at[o], device_id={'w': dst}, device_id_type=pl.DeviceIdType.MESH))
        return out

    def wait_sends(kk):
        for o, copy in enumerate(sends(kk)):
            if o == 0:
                copy.wait()
            else:
                copy.wait_send()

    for copy in fetches(0):
        copy.start()

    @pl.loop(0, KK)
    def _(kk):
        slot = lax.rem(kk, 2)

        @pl.when(kk + 1 < KK)
        def _():
            for copy in fetches(kk + 1):
                copy.start()

        for copy in fetches(kk):
            copy.wait()

        @pl.when(kk >= 2)
        def _():
            wait_sends(kk - 2)
            for copy in stores(kk - 2):
                copy.wait()

        sums = []
        for par in range(2):
            rows = slice(par * (WAVES // 2), (par + 1) * (WAVES // 2))
            x = jnp.concatenate([fbuf[slot, 0, rows, :], fbuf[slot, 1, rows, :]], axis=0)
            x_hi, x_lo = split(x)
            sums.append(dot3(dft[par, 0], dft[par, 1], x_hi, x_lo, ((1,), (0,))))
        first, second = sums[0] + sums[1], sums[0] - sums[1]
        gbuf[slot, :, 0:HALF] = first.T
        gbuf[slot, :, HALF:LONS] = second.T
        for copy in stores(kk):
            copy.start()
        first, second = first * first, second * second
        for par, y in enumerate((first + second, first - second)):
            y_hi, y_lo = split(y)
            h = dot3(dft_t[par, 0], dft_t[par, 1], y_hi, y_lo, ((1,), (0,))) * weight[...]
            stage[slot, par, 0] = h[0:WAVES // 2]
            stage[slot, par, 1] = h[WAVES // 2:]
        for copy in sends(kk):
            copy.start()

    for kk in (KK - 2, KK - 1):
        wait_sends(kk)
        for copy in stores(kk):
            copy.wait()
    for o in range(1, DEVS):
        part = recv.at[lax.rem(me - o + DEVS, DEVS)]
        pltpu.make_async_copy(part, part, rsem.at[o]).wait()


def forward_legendre(h_in, leg, out, hbuf, lbuf, obuf, hsem, lsem, osem):
    me = lax.axis_index('w')

    def fetch_leg(t):
        slot = lax.rem(t, NB)
        return pltpu.make_async_copy(leg.at[me * OWN + own_wave(t)], lbuf.at[slot], lsem.at[slot])

    def fetch_h(c):
        slot = lax.rem(c, 2)
        row = pl.multiple_of(lax.rem(c, 4) * CHUNK, CHUNK)
        return pltpu.make_async_copy(h_in.at[:, lax.div(c, 4), :, :, pl.ds(row, CHUNK), :], hbuf.at[slot], hsem.at[slot])

    def store(t):
        slot = lax.rem(t, 2)
        return pltpu.make_async_copy(obuf.at[slot], out.at[own_wave(t)], osem.at[slot])

    fetch_h(0).start()
    for t in range(NB):
        fetch_leg(t).start()

    @pl.loop(0, OWN // CHUNK)
    def _(c):
        @pl.when(c + 1 < OWN // CHUNK)
        def _():
            fetch_h(c + 1).start()

        fetch_h(c).wait()
        hslot = lax.rem(c, 2)

        @pl.loop(0, CHUNK)
        def _(i):
            t = c * CHUNK + i
            rows = []
            for r in range(2):
                parts = []
                for d in range(DEVS):
                    parts.append(jnp.concatenate([hbuf[hslot, d, r, kk, pl.ds(i, 1), :] for kk in range(KK)], axis=0))
                for q in range(QQ):
                    rows.append(jnp.concatenate([p[:, q * LAT:(q + 1) * LAT] for p in parts], axis=1))
            h_hi, h_lo = split(jnp.concatenate(rows, axis=0))
            fetch_leg(t).wait()
            l_hi, l_lo = split(lbuf[lax.rem(t, NB)])

            @pl.when(t >= 2)
            def _():
                store(t - 2).wait()

            s = dot3(h_hi, h_lo, l_hi, l_lo, ((1,), (1,)))
            obuf[lax.rem(t, 2)] = s.reshape(2, LEVS, WAVES)
            store(t).start()

            @pl.when(t + NB < OWN)
            def _():
                fetch_leg(t + NB).start()

    store(OWN - 2).wait()
    store(OWN - 1).wait()


def dft_tables():
    n = np.arange(HALF)[:, None]
    tabs = []
    for par in range(2):
        m = np.arange(par, WAVES, 2)[None, :]
        ang = 2 * np.pi * ((m * n) % LONS) / LONS
        tabs.append(np.concatenate([np.cos(ang), -np.sin(ang)], axis=1))
    back = np.stack(tabs)
    scale = np.full((2, 1, WAVES), 2.0 / LONS)
    scale[0, 0, 0] = 1.0 / LONS
    scale[0, 0, WAVES // 2] = 0.0

    def halves(x):
        x = x.astype(np.float32)
        hi = x.astype(jnp.bfloat16)
        return np.stack([hi, (x - hi.astype(np.float32)).astype(jnp.bfloat16)], axis=1)

    return halves(back * scale), halves(np.swapaxes(back, 1, 2))


ANY = pl.BlockSpec(memory_space=pl.ANY)
VM = pl.BlockSpec(memory_space=pltpu.VMEM)
DMA = pltpu.SemaphoreType.DMA
LIMIT = 60 * 1024 * 1024


def solution(mesh):
    dft, dft_t = dft_tables()

    def per_device(coef, legendre, gauss_weight):
        me = lax.axis_index('w')
        own = lax.dynamic_slice_in_dim(gauss_weight, me * LAT, LAT, axis=0)
        weight = jnp.tile(own, QQ)[None, :]
        fourier = pl.pallas_call(
            inverse_legendre,
            out_shape=jax.ShapeDtypeStruct((ROWS, WAVES, LANES), F32),
            in_specs=[ANY, ANY],
            out_specs=ANY,
            scratch_shapes=[
                pltpu.VMEM((NB, 2, LEVS, WAVES), F32),
                pltpu.VMEM((NB, WAVES, LATS), F32),
                pltpu.VMEM((2, DEVS, ROWS, CHUNK, LANES), F32),
                DMA((NB,)), DMA((NB,)), DMA((2, DEVS)), DMA((2, DEVS)),
            ],
            compiler_params=pltpu.CompilerParams(collective_id=0, has_side_effects=True, vmem_limit_bytes=LIMIT),
            name='inverse_legendre',
        )(coef, legendre)
        grid, hats = pl.pallas_call(
            longitudes,
            out_shape=(jax.ShapeDtypeStruct((LEVS, LAT, LONS), F32), jax.ShapeDtypeStruct((DEVS, 2, 2, KK, OWN // 2, LANES), F32)),
            in_specs=[ANY, VM, VM, VM],
            out_specs=(ANY, ANY),
            scratch_shapes=[
                pltpu.VMEM((2, 2, WAVES, LANES), F32),
                pltpu.VMEM((2, LANES, LONS), F32),
                pltpu.VMEM((2, 2, 2, WAVES // 2, LANES), F32),
                DMA((2, 2)), DMA((2, QQ)), DMA((2, DEVS)), DMA((DEVS,)),
            ],
            compiler_params=pltpu.CompilerParams(collective_id=1, has_side_effects=True, vmem_limit_bytes=LIMIT),
            name='longitudes',
        )(fourier, dft, dft_t, weight)
        spec_out = pl.pallas_call(
            forward_legendre,
            out_shape=jax.ShapeDtypeStruct((OWN, 2, LEVS, WAVES), F32),
            in_specs=[ANY, ANY],
            out_specs=ANY,
            scratch_shapes=[
                pltpu.VMEM((2, DEVS, 2, KK, CHUNK, LANES), F32),
                pltpu.VMEM((NB, WAVES, LATS), F32),
                pltpu.VMEM((2, 2, LEVS, WAVES), F32),
                DMA((2,)), DMA((NB,)), DMA((2,)),
            ],
            compiler_params=pltpu.CompilerParams(vmem_limit_bytes=LIMIT),
            name='forward_legendre',
        )(hats, legendre)
        return grid, spec_out

    return jax.shard_map(per_device, mesh=mesh, in_specs=(P('w', None, 'lev', None), P(None, None, None), P(None)), out_specs=(P('lev', 'w', None), P('w', None, 'lev', None)), check_vma=False)
```

```python
import functools

import jax
import jax.numpy as jnp
import numpy as np
from jax import lax
from jax.experimental import pallas as pl
from jax.experimental.pallas import tpu as pltpu
from jax.sharding import PartitionSpec as P

DEVS = 8
WAVES = 512
OWN = WAVES // DEVS
LATS = 768
LAT = LATS // DEVS
LEVS = 32
LONS = 1024
HALF = LONS // 2
KK = 8
QQ = 4
LANES = QQ * LAT
CHUNK = 8
NB = 3
CHUNKS = OWN // CHUNK
EARLY = 2
AHEAD = 3
EARLY_WAVES = OWN - CHUNK
ROWS = 2 * KK
BF = jnp.bfloat16
F32 = jnp.float32


def split(x):
    hi = x.astype(BF)
    return hi, (x - hi.astype(F32)).astype(BF)


def dot3(a_hi, a_lo, b_hi, b_lo, dims):
    mm = functools.partial(lax.dot_general, dimension_numbers=(dims, ((), ())), preferred_element_type=F32)
    return mm(a_hi, b_hi) + (mm(a_hi, b_lo) + mm(a_lo, b_hi))


def dot_stacked(a, b, dims):
    rows = a.shape[0]
    (a_hi, a_lo), (b_hi, b_lo) = split(a), split(b)
    mm = functools.partial(lax.dot_general, dimension_numbers=(dims, ((), ())), preferred_element_type=F32)
    both = mm(jnp.concatenate([a_hi, a_lo], axis=0), b_hi)
    return both[:rows] + (both[rows:] + mm(a_hi, b_lo))


def barrier_all(me):
    sem = pltpu.get_barrier_semaphore()
    for o in range(1, DEVS):
        pl.semaphore_signal(sem, inc=1, device_id={'w': lax.rem(me + o, DEVS)}, device_id_type=pl.DeviceIdType.MESH)
    pl.semaphore_wait(sem, DEVS - 1)


def own_wave(t):
    return 2 * lax.rem(t, OWN // 2) + lax.div(t, OWN // 2)


def inverse_legendre(coef, leg, recv, cbuf, lbuf, stage, csem, lsem, ssem, rsem):
    me = lax.axis_index('w')
    barrier_all(me)

    def fetches(t):
        slot = lax.rem(t, NB)
        m = own_wave(t)
        return (pltpu.make_async_copy(coef.at[m], cbuf.at[slot], csem.at[slot]), pltpu.make_async_copy(leg.at[me * OWN + m], lbuf.at[slot], lsem.at[slot]))

    def sends(c):
        slot = lax.rem(c, 2)
        row = lax.div(c, 4) * (WAVES // 2) + me * (OWN // 2) + lax.rem(c, 4) * CHUNK
        row = pl.multiple_of(row, CHUNK)
        out = []
        for o in range(DEVS):
            dst = lax.rem(me + o, DEVS)
            src_ref, dst_ref = stage.at[slot, dst], recv.at[:, pl.ds(row, CHUNK), :]
            if o == 0:
                out.append(pltpu.make_async_copy(src_ref, dst_ref, ssem.at[slot, 0]))
            else:
                out.append(pltpu.make_async_remote_copy(src_ref=src_ref, dst_ref=dst_ref, send_sem=ssem.at[slot, o], recv_sem=rsem.at[lax.div(c, 4), o], device_id={'w': dst}, device_id_type=pl.DeviceIdType.MESH))
        return out

    def wait_sends(c):
        for o, copy in enumerate(sends(c)):
            if o == 0:
                copy.wait()
            else:
                copy.wait_send()

    for t in range(NB):
        for copy in fetches(t):
            copy.start()

    @pl.loop(0, OWN // CHUNK)
    def _(c):
        slot = lax.rem(c, 2)

        @pl.when(c >= 2)
        def _():
            wait_sends(c - 2)

        @pl.loop(0, CHUNK)
        def _(i):
            t = c * CHUNK + i
            for copy in fetches(t):
                copy.wait()
            buf = lax.rem(t, NB)
            f = dot_stacked(cbuf[buf].reshape(2 * LEVS, WAVES), lbuf[buf], ((1,), (0,)))

            @pl.when(t + NB < OWN)
            def _():
                for copy in fetches(t + NB):
                    copy.start()

            for d in range(DEVS):
                cols = f[:, d * LAT:(d + 1) * LAT]
                for r in range(2):
                    row = r * LEVS
                    packed = jnp.concatenate([cols[row + q * KK:row + (q + 1) * KK] for q in range(QQ)], axis=1)
                    for h in range(KK):
                        stage[slot, d, r * KK + h, pl.ds(i, 1), :] = packed[h:h + 1]

        for copy in sends(c):
            copy.start()

    wait_sends(OWN // CHUNK - 2)
    wait_sends(OWN // CHUNK - 1)
    for o in range(1, DEVS):
        src = lax.rem(me - o + DEVS, DEVS)
        for par in range(2):
            part = recv.at[:, pl.ds(pl.multiple_of(par * (WAVES // 2) + src * (OWN // 2), OWN // 2), OWN // 2), :]
            pltpu.make_async_copy(part, part, rsem.at[par, o]).wait()


def gather_rows(hbuf, i):
    rows = []
    for r in range(2):
        parts = [jnp.concatenate([hbuf[d, r, kk, pl.ds(i, 1), :] for kk in range(KK)], axis=0) for d in range(DEVS)]
        for q in range(QQ):
            rows.append(jnp.concatenate([p[:, q * LAT:(q + 1) * LAT] for p in parts], axis=1))
    return jnp.concatenate(rows, axis=0)


def longitudes(f_in, leg, dft, dft_t, weight, grid_out, spec_out, last_out, fbuf, gbuf, hsend, hrecv, lbuf, obuf, fsem, gsem, ssem, asem, bsem, lsem, osem):
    me = lax.axis_index('w')
    barrier_all(me)

    def fetches(kk):
        slot = lax.rem(kk, 2)
        return [pltpu.make_async_copy(f_in.at[r * KK + kk], fbuf.at[slot, r], fsem.at[slot, r]) for r in range(2)]

    def fetch_leg(t):
        slot = lax.rem(t, NB)
        return pltpu.make_async_copy(leg.at[me * OWN + own_wave(t)], lbuf.at[slot], lsem.at[slot])

    def stores(kk):
        slot = lax.rem(kk, 2)
        return [pltpu.make_async_copy(gbuf.at[slot, pl.ds(q * LAT, LAT)], grid_out.at[q * KK + kk], gsem.at[slot, q]) for q in range(QQ)]

    def send(o, src_ref, dst_ref, sem):
        if o == 0:
            pltpu.make_async_copy(src_ref, dst_ref, sem).start()
        else:
            pltpu.make_async_remote_copy(src_ref=src_ref, dst_ref=dst_ref, send_sem=ssem.at[o], recv_sem=sem, device_id={'w': lax.rem(me + o, DEVS)}, device_id_type=pl.DeviceIdType.MESH).start()

    def dst_rows(o, row, size):
        return pl.ds(pl.multiple_of(lax.rem(me + o, DEVS) * (OWN // 2) + row, CHUNK), size)

    def send_levels(kk):
        for o in range(DEVS):
            send(o, hsend.at[:, :, kk, dst_rows(o, 0, OWN // 2), :], hrecv.at[me, :, :, kk], asem.at[o])

    def chunk_at(ref, c):
        row = pl.multiple_of(lax.rem(c, 4) * CHUNK, CHUNK)
        return ref.at[lax.div(c, 4), :, pl.ds(EARLY, KK - EARLY), pl.ds(row, CHUNK), :]

    def send_chunk(c):
        row = lax.rem(c, 4) * CHUNK
        for o in range(DEVS):
            send(o, hsend.at[lax.div(c, 4), :, pl.ds(EARLY, KK - EARLY), dst_rows(o, row, CHUNK), :], chunk_at(hrecv.at[me], c), bsem.at[c, o])

    def arrived(c):
        for o in range(DEVS):
            part = chunk_at(hrecv.at[lax.rem(me - o + DEVS, DEVS)], c)
            pltpu.make_async_copy(part, part, bsem.at[c, o]).wait()

    def store(t):
        slot = lax.rem(t, 2)
        return pltpu.make_async_copy(obuf.at[slot], spec_out.at[t], osem.at[slot])

    for copy in fetches(0):
        copy.start()
    for t in range(NB):
        fetch_leg(t).start()

    @pl.loop(0, KK)
    def _(kk):
        slot = lax.rem(kk, 2)

        @pl.when(kk + 1 < KK)
        def _():
            for copy in fetches(kk + 1):
                copy.start()

        for copy in fetches(kk):
            copy.wait()

        @pl.when(kk >= 2)
        def _():
            for copy in stores(kk - 2):
                copy.wait()

        sums = []
        for par in range(2):
            rows = slice(par * (WAVES // 2), (par + 1) * (WAVES // 2))
            x = jnp.concatenate([fbuf[slot, 0, rows, :], fbuf[slot, 1, rows, :]], axis=0)
            x_hi, x_lo = split(x)
            sums.append(dot3(dft[par, 0], dft[par, 1], x_hi, x_lo, ((1,), (0,))))
        first, second = sums[0] + sums[1], sums[0] - sums[1]
        gbuf[slot, :, 0:HALF] = first.T
        gbuf[slot, :, HALF:LONS] = second.T
        for copy in stores(kk):
            copy.start()
        first, second = first * first, second * second
        for par, y in enumerate((first + second, first - second)):
            y_hi, y_lo = split(y)
            h = dot3(dft_t[par, 0], dft_t[par, 1], y_hi, y_lo, ((1,), (0,))) * weight[...]
            hsend[par, 0, kk] = h[0:WAVES // 2]
            hsend[par, 1, kk] = h[WAVES // 2:]

        @pl.when(kk < EARLY)
        def _():
            send_levels(kk)

    for c in range(AHEAD):
        send_chunk(c)
    for kk in (KK - 2, KK - 1):
        for copy in stores(kk):
            copy.wait()
    for o in range(DEVS):
        part = hrecv.at[lax.rem(me - o + DEVS, DEVS), :, :, pl.ds(0, EARLY)]
        pltpu.make_async_copy(part, part, asem.at[o]).wait()

    @pl.loop(0, CHUNKS - 1)
    def _(c):
        arrived(c)

        @pl.when(c + AHEAD < CHUNKS)
        def _():
            send_chunk(c + AHEAD)

        par, row = lax.div(c, 4), lax.rem(c, 4) * CHUNK

        @pl.loop(0, CHUNK)
        def _(i):
            t = c * CHUNK + i
            h = gather_rows(hrecv.at[:, par], row + i)
            fetch_leg(t).wait()

            @pl.when(t >= 2)
            def _():
                store(t - 2).wait()

            obuf[lax.rem(t, 2)] = dot_stacked(h, lbuf[lax.rem(t, NB)], ((1,), (1,))).reshape(2, LEVS, WAVES)
            store(t).start()

            @pl.when(t + NB < EARLY_WAVES)
            def _():
                fetch_leg(t + NB).start()

    arrived(CHUNKS - 1)
    last = pltpu.make_async_copy(hrecv.at[:, 1, :, :, pl.ds(3 * CHUNK, CHUNK), :], last_out, asem.at[0])
    last.start()
    store(EARLY_WAVES - 2).wait()
    store(EARLY_WAVES - 1).wait()
    for o in range(1, DEVS):
        part = hsend.at[:, :, :, dst_rows(o, 0, OWN // 2), :]
        pltpu.make_async_copy(part, part, ssem.at[o]).wait()
    last.wait()


def finish(h_in, leg, grid_in, spec_in, grid_out, spec_out, hbuf, lbuf, obuf, gbuf, sbuf, hsem, lsem, osem, gsem, ssem, tsem):
    me = lax.axis_index('w')
    fetch_h = pltpu.make_async_copy(h_in, hbuf, hsem)
    fetch_h.start()

    def fetch_leg(i):
        return pltpu.make_async_copy(leg.at[me * OWN + own_wave(EARLY_WAVES + i)], lbuf.at[i], lsem.at[i])

    def grid_copy(i, back):
        hbm = (grid_out if back else grid_in).at[pl.ds(i * QQ, QQ)]
        return pltpu.make_async_copy(gbuf.at[i], hbm, gsem.at[1, i]) if back else pltpu.make_async_copy(hbm, gbuf.at[i], gsem.at[0, i])

    def spec_fetch(i):
        return pltpu.make_async_copy(spec_in.at[pl.ds(i * 7, 7)], sbuf.at[pl.ds(i * 7, 7)], ssem.at[i])

    def spec_store(t):
        return pltpu.make_async_copy(sbuf.at[t], spec_out.at[own_wave(t)], tsem.at[t])

    def store(i):
        return pltpu.make_async_copy(obuf.at[i], spec_out.at[own_wave(EARLY_WAVES + i)], osem.at[i])

    fetch_leg(0).start()
    fetch_leg(1).start()
    for i in range(CHUNK):
        grid_copy(i, False).start()
        spec_fetch(i).start()
        if i + 2 < CHUNK:
            fetch_leg(i + 2).start()
    fetch_h.wait()

    @pl.loop(0, CHUNK)
    def _(i):
        h = gather_rows(hbuf, i)
        fetch_leg(i).wait()
        obuf[i] = dot_stacked(h, lbuf[i], ((1,), (1,))).reshape(2, LEVS, WAVES)
        store(i).start()
        grid_copy(i, False).wait()
        grid_copy(i, True).start()
        spec_fetch(i).wait()
        for j in range(7):
            spec_store(i * 7 + j).start()

    @pl.loop(0, CHUNK)
    def _(i):
        store(i).wait()
        grid_copy(i, True).wait()
        for j in range(7):
            spec_store(i * 7 + j).wait()


def dft_tables():
    n = np.arange(HALF)[:, None]
    tabs = []
    for par in range(2):
        m = np.arange(par, WAVES, 2)[None, :]
        ang = 2 * np.pi * ((m * n) % LONS) / LONS
        tabs.append(np.concatenate([np.cos(ang), -np.sin(ang)], axis=1))
    back = np.stack(tabs)
    scale = np.full((2, 1, WAVES), 2.0 / LONS)
    scale[0, 0, 0] = 1.0 / LONS
    scale[0, 0, WAVES // 2] = 0.0

    def halves(x):
        x = x.astype(np.float32)
        hi = x.astype(jnp.bfloat16)
        return np.stack([hi, (x - hi.astype(np.float32)).astype(jnp.bfloat16)], axis=1)

    return halves(back * scale), halves(np.swapaxes(back, 1, 2))


ANY = pl.BlockSpec(memory_space=pl.ANY)
VM = pl.BlockSpec(memory_space=pltpu.VMEM)
DMA = pltpu.SemaphoreType.DMA
LIMIT = 60 * 1024 * 1024


def solution(mesh):
    dft, dft_t = dft_tables()

    def per_device(coef, legendre, gauss_weight):
        me = lax.axis_index('w')
        own = lax.dynamic_slice_in_dim(gauss_weight, me * LAT, LAT, axis=0)
        weight = jnp.tile(own, QQ)[None, :]
        fourier = pl.pallas_call(
            inverse_legendre,
            out_shape=jax.ShapeDtypeStruct((ROWS, WAVES, LANES), F32),
            in_specs=[ANY, ANY],
            out_specs=ANY,
            scratch_shapes=[
                pltpu.VMEM((NB, 2, LEVS, WAVES), F32),
                pltpu.VMEM((NB, WAVES, LATS), F32),
                pltpu.VMEM((2, DEVS, ROWS, CHUNK, LANES), F32),
                DMA((NB,)), DMA((NB,)), DMA((2, DEVS)), DMA((2, DEVS)),
            ],
            compiler_params=pltpu.CompilerParams(collective_id=0, has_side_effects=True, vmem_limit_bytes=LIMIT),
            name='inverse_legendre',
        )(coef, legendre)
        grid_mid, spec_mid, last = pl.pallas_call(
            longitudes,
            out_shape=(
                jax.ShapeDtypeStruct((LEVS, LAT, LONS), F32),
                jax.ShapeDtypeStruct((EARLY_WAVES, 2, LEVS, WAVES), F32),
                jax.ShapeDtypeStruct((DEVS, 2, KK, CHUNK, LANES), F32),
            ),
            in_specs=[ANY, ANY, VM, VM, VM],
            out_specs=(ANY, ANY, ANY),
            scratch_shapes=[
                pltpu.VMEM((2, 2, WAVES, LANES), F32),
                pltpu.VMEM((2, LANES, LONS), F32),
                pltpu.VMEM((2, 2, KK, WAVES // 2, LANES), F32),
                pltpu.VMEM((DEVS, 2, 2, KK, OWN // 2, LANES), F32),
                pltpu.VMEM((NB, WAVES, LATS), F32),
                pltpu.VMEM((2, 2, LEVS, WAVES), F32),
                DMA((2, 2)), DMA((2, QQ)), DMA((DEVS,)), DMA((DEVS,)), DMA((CHUNKS, DEVS)), DMA((NB,)), DMA((2,)),
            ],
            compiler_params=pltpu.CompilerParams(collective_id=1, has_side_effects=True, vmem_limit_bytes=LIMIT),
            name='longitudes',
        )(fourier, legendre, dft, dft_t, weight)
        grid, spec_out = pl.pallas_call(
            finish,
            out_shape=(jax.ShapeDtypeStruct((LEVS, LAT, LONS), F32), jax.ShapeDtypeStruct((OWN, 2, LEVS, WAVES), F32)),
            in_specs=[ANY, ANY, ANY, ANY],
            out_specs=(ANY, ANY),
            scratch_shapes=[
                pltpu.VMEM((DEVS, 2, KK, CHUNK, LANES), F32),
                pltpu.VMEM((CHUNK, WAVES, LATS), F32),
                pltpu.VMEM((CHUNK, 2, LEVS, WAVES), F32),
                pltpu.VMEM((CHUNK, QQ, LAT, LONS), F32),
                pltpu.VMEM((EARLY_WAVES, 2, LEVS, WAVES), F32),
                DMA, DMA((CHUNK,)), DMA((CHUNK,)), DMA((2, CHUNK)), DMA((CHUNK,)), DMA((EARLY_WAVES,)),
            ],
            compiler_params=pltpu.CompilerParams(vmem_limit_bytes=LIMIT),
            name='finish',
        )(last, legendre, grid_mid, spec_mid)
        return grid, spec_out

    return jax.shard_map(per_device, mesh=mesh, in_specs=(P('w', None, 'lev', None), P(None, None, None), P(None)), out_specs=(P('lev', 'w', None), P('w', None, 'lev', None)), check_vma=False)
```

```python
import functools

import jax
import jax.numpy as jnp
import numpy as np
from jax import lax
from jax.experimental import pallas as pl
from jax.experimental.pallas import tpu as pltpu
from jax.sharding import PartitionSpec as P

DEVS = 8
WAVES = 512
OWN = WAVES // DEVS
LATS = 768
LAT = LATS // DEVS
LEVS = 32
LONS = 1024
HALF = LONS // 2
KK = 8
QQ = 4
LANES = QQ * LAT
CHUNK = 8
NB = 3
CHUNKS = OWN // CHUNK
FIRST = 4
EARLY = 2
AHEAD = 3
EARLY_WAVES = OWN - CHUNK
BF = jnp.bfloat16
F32 = jnp.float32


def split(x):
    hi = x.astype(BF)
    return hi, (x - hi.astype(F32)).astype(BF)


def dot3(a_hi, a_lo, b_hi, b_lo, dims):
    mm = functools.partial(lax.dot_general, dimension_numbers=(dims, ((), ())), preferred_element_type=F32)
    return mm(a_hi, b_hi) + (mm(a_hi, b_lo) + mm(a_lo, b_hi))


def dot_stacked(a, b, dims):
    rows = a.shape[0]
    (a_hi, a_lo), (b_hi, b_lo) = split(a), split(b)
    mm = functools.partial(lax.dot_general, dimension_numbers=(dims, ((), ())), preferred_element_type=F32)
    both = mm(jnp.concatenate([a_hi, a_lo], axis=0), b_hi)
    return both[:rows] + (both[rows:] + mm(a_hi, b_lo))


def barrier_all(me):
    sem = pltpu.get_barrier_semaphore()
    for o in range(1, DEVS):
        pl.semaphore_signal(sem, inc=1, device_id={'w': lax.rem(me + o, DEVS)}, device_id_type=pl.DeviceIdType.MESH)
    pl.semaphore_wait(sem, DEVS - 1)


def own_wave(t):
    return 2 * lax.rem(t, OWN // 2) + lax.div(t, OWN // 2)


def gather_rows(hbuf, i):
    rows = []
    for r in range(2):
        parts = [jnp.concatenate([hbuf[d, kk, r, pl.ds(i, 1), :] for kk in range(KK)], axis=0) for d in range(DEVS)]
        for q in range(QQ):
            rows.append(jnp.concatenate([p[:, q * LAT:(q + 1) * LAT] for p in parts], axis=1))
    return jnp.concatenate(rows, axis=0)


def transform(coef, leg, dft, dft_t, weight, frecv, grid_out, spec_out, last_out, cbuf, lbuf, fbuf, gbuf, both, hrecv, obuf, csem, lsem, fsem, gsem, osem, fs1, fr1, fs2, fr2, ssem, asem, bsem):
    me = lax.axis_index('w')
    barrier_all(me)

    def fetch_leg(t):
        slot = lax.rem(t, NB)
        return pltpu.make_async_copy(leg.at[me * OWN + own_wave(t)], lbuf.at[slot], lsem.at[slot])

    def fetch_coef(t):
        slot = lax.rem(t, NB)
        return pltpu.make_async_copy(coef.at[own_wave(t)], cbuf.at[slot], csem.at[slot])

    def target(o):
        return lax.rem(me + o, DEVS)

    def source(o):
        return lax.rem(me - o + DEVS, DEVS)

    def block(d, row=0, size=OWN):
        return pl.ds(pl.multiple_of(d * OWN + row, CHUNK), size)

    def move(o, src_ref, dst_ref, send_sem, recv_sem):
        if o == 0:
            pltpu.make_async_copy(src_ref, dst_ref, recv_sem).start()
        else:
            pltpu.make_async_remote_copy(src_ref=src_ref, dst_ref=dst_ref, send_sem=send_sem, recv_sem=recv_sem, device_id={'w': target(o)}, device_id_type=pl.DeviceIdType.MESH).start()

    def wait_for(part, sem):
        pltpu.make_async_copy(part, part, sem).wait()

    for t in range(NB):
        fetch_leg(t).start()
        fetch_coef(t).start()

    @pl.loop(0, CHUNKS)
    def _(c):
        @pl.loop(0, CHUNK)
        def _(i):
            t = c * CHUNK + i
            fetch_leg(t).wait()
            fetch_coef(t).wait()
            buf = lax.rem(t, NB)
            f = dot_stacked(cbuf[buf].reshape(2 * LEVS, WAVES), lbuf[buf], ((1,), (0,)))

            @pl.when(t + NB < OWN)
            def _():
                fetch_leg(t + NB).start()
                fetch_coef(t + NB).start()

            for d in range(DEVS):
                cols = f[:, d * LAT:(d + 1) * LAT]
                for r in range(2):
                    row = r * LEVS
                    packed = jnp.concatenate([cols[row + q * KK:row + (q + 1) * KK] for q in range(QQ)], axis=1)
                    for kk in range(KK):
                        both[kk, r, pl.ds(d * OWN + t, 1), :] = packed[kk:kk + 1]

        for o in range(DEVS):
            move(o, both.at[pl.ds(0, FIRST), :, block(target(o), c * CHUNK, CHUNK), :], frecv.at[pl.ds(0, FIRST), :, block(me, c * CHUNK, CHUNK), :], fs1.at[o], fr1.at[o])

    for kk in range(FIRST, KK):
        for o in range(DEVS):
            move(o, both.at[kk, :, block(target(o)), :], frecv.at[kk, :, block(me), :], fs2.at[kk, o], fr2.at[kk, o])
    for t in range(NB):
        fetch_leg(t).start()

    def stores(kk):
        slot = lax.rem(kk, 2)
        return [pltpu.make_async_copy(gbuf.at[slot, pl.ds(q * LAT, LAT)], grid_out.at[q * KK + kk], gsem.at[slot, q]) for q in range(QQ)]

    def dst_rows(o, row, size):
        return pl.ds(pl.multiple_of(target(o) * (OWN // 2) + row, CHUNK), size)

    def send_levels(kk):
        for o in range(DEVS):
            for par in range(2):
                move(o, both.at[kk, :, dst_rows(o, par * (WAVES // 2), OWN // 2), :], hrecv.at[me, par, kk], ssem.at[o], asem.at[o])

    def chunk_at(ref, c):
        row = pl.multiple_of(lax.rem(c, 4) * CHUNK, CHUNK)
        return ref.at[lax.div(c, 4), pl.ds(EARLY, KK - EARLY), :, pl.ds(row, CHUNK), :]

    def send_chunk(c):
        row = lax.div(c, 4) * (WAVES // 2) + lax.rem(c, 4) * CHUNK
        for o in range(DEVS):
            move(o, both.at[pl.ds(EARLY, KK - EARLY), :, dst_rows(o, row, CHUNK), :], chunk_at(hrecv.at[me], c), ssem.at[o], bsem.at[c, o])

    def arrived(c):
        for o in range(DEVS):
            wait_for(chunk_at(hrecv.at[source(o)], c), bsem.at[c, o])

    def store(t):
        slot = lax.rem(t, 2)
        return pltpu.make_async_copy(obuf.at[slot], spec_out.at[t], osem.at[slot])

    @pl.loop(0, KK)
    def _(kk):
        slot = lax.rem(kk, 2)

        @pl.when(kk == 0)
        def _():
            for o in range(DEVS):
                wait_for(frecv.at[pl.ds(0, FIRST), :, block(source(o)), :], fr1.at[o])
            for o in range(1, DEVS):
                wait_for(both.at[pl.ds(0, FIRST), :, block(target(o)), :], fs1.at[o])

        @pl.when(kk >= FIRST)
        def _():
            for o in range(DEVS):
                wait_for(frecv.at[kk, :, block(source(o)), :], fr2.at[kk, o])
            for o in range(1, DEVS):
                wait_for(both.at[kk, :, block(target(o)), :], fs2.at[kk, o])

        fetch = pltpu.make_async_copy(frecv.at[kk], fbuf, fsem)
        fetch.start()
        fetch.wait()

        @pl.when(kk >= 2)
        def _():
            for copy in stores(kk - 2):
                copy.wait()

        sums = []
        for par in range(2):
            x = jnp.concatenate([fbuf[r, d * OWN + par * (OWN // 2):d * OWN + (par + 1) * (OWN // 2), :] for r in range(2) for d in range(DEVS)], axis=0)
            x_hi, x_lo = split(x)
            sums.append(dot3(dft[par, 0], dft[par, 1], x_hi, x_lo, ((1,), (0,))))
        first, second = sums[0] + sums[1], sums[0] - sums[1]
        gbuf[slot, :, 0:HALF] = first.T
        gbuf[slot, :, HALF:LONS] = second.T
        for copy in stores(kk):
            copy.start()
        first, second = first * first, second * second
        for par, y in enumerate((first + second, first - second)):
            y_hi, y_lo = split(y)
            h = dot3(dft_t[par, 0], dft_t[par, 1], y_hi, y_lo, ((1,), (0,))) * weight[...]
            for r in range(2):
                both[kk, r, par * (WAVES // 2):(par + 1) * (WAVES // 2), :] = h[r * (WAVES // 2):(r + 1) * (WAVES // 2)]

        @pl.when(kk < EARLY)
        def _():
            send_levels(kk)

    for c in range(AHEAD):
        send_chunk(c)
    for kk in (KK - 2, KK - 1):
        for copy in stores(kk):
            copy.wait()
    for o in range(DEVS):
        wait_for(hrecv.at[source(o), :, pl.ds(0, EARLY)], asem.at[o])

    @pl.loop(0, CHUNKS - 1)
    def _(c):
        arrived(c)

        @pl.when(c + AHEAD < CHUNKS)
        def _():
            send_chunk(c + AHEAD)

        par, row = lax.div(c, 4), lax.rem(c, 4) * CHUNK

        @pl.loop(0, CHUNK)
        def _(i):
            t = c * CHUNK + i
            h = gather_rows(hrecv.at[:, par], row + i)
            fetch_leg(t).wait()

            @pl.when(t >= 2)
            def _():
                store(t - 2).wait()

            obuf[lax.rem(t, 2)] = dot_stacked(h, lbuf[lax.rem(t, NB)], ((1,), (1,))).reshape(2, LEVS, WAVES)
            store(t).start()

            @pl.when(t + NB < EARLY_WAVES)
            def _():
                fetch_leg(t + NB).start()

    arrived(CHUNKS - 1)
    last = pltpu.make_async_copy(hrecv.at[:, 1, :, :, pl.ds(3 * CHUNK, CHUNK), :], last_out, fsem)
    last.start()
    store(EARLY_WAVES - 2).wait()
    store(EARLY_WAVES - 1).wait()
    for o in range(1, DEVS):
        wait_for(both.at[:, :, block(target(o)), :], ssem.at[o])
    last.wait()


def finish(h_in, leg, grid_in, spec_in, grid_out, spec_out, hbuf, lbuf, obuf, gbuf, sbuf, hsem, lsem, osem, gsem, ssem, tsem):
    me = lax.axis_index('w')
    fetch_h = pltpu.make_async_copy(h_in, hbuf, hsem)
    fetch_h.start()

    def fetch_leg(i):
        return pltpu.make_async_copy(leg.at[me * OWN + own_wave(EARLY_WAVES + i)], lbuf.at[i], lsem.at[i])

    def grid_copy(i, back):
        hbm = (grid_out if back else grid_in).at[pl.ds(i * QQ, QQ)]
        return pltpu.make_async_copy(gbuf.at[i], hbm, gsem.at[1, i]) if back else pltpu.make_async_copy(hbm, gbuf.at[i], gsem.at[0, i])

    def spec_fetch(i):
        return pltpu.make_async_copy(spec_in.at[pl.ds(i * 7, 7)], sbuf.at[pl.ds(i * 7, 7)], ssem.at[i])

    def spec_store(t):
        return pltpu.make_async_copy(sbuf.at[t], spec_out.at[own_wave(t)], tsem.at[t])

    def store(i):
        return pltpu.make_async_copy(obuf.at[i], spec_out.at[own_wave(EARLY_WAVES + i)], osem.at[i])

    fetch_leg(0).start()
    fetch_leg(1).start()
    for i in range(CHUNK):
        grid_copy(i, False).start()
        spec_fetch(i).start()
        if i + 2 < CHUNK:
            fetch_leg(i + 2).start()
    fetch_h.wait()

    @pl.loop(0, CHUNK)
    def _(i):
        h = gather_rows(hbuf, i)
        fetch_leg(i).wait()
        obuf[i] = dot_stacked(h, lbuf[i], ((1,), (1,))).reshape(2, LEVS, WAVES)
        store(i).start()
        grid_copy(i, False).wait()
        grid_copy(i, True).start()
        spec_fetch(i).wait()
        for j in range(7):
            spec_store(i * 7 + j).start()

    @pl.loop(0, CHUNK)
    def _(i):
        store(i).wait()
        grid_copy(i, True).wait()
        for j in range(7):
            spec_store(i * 7 + j).wait()


def dft_tables():
    n = np.arange(HALF)[:, None]
    tabs = []
    for par in range(2):
        m = np.arange(par, WAVES, 2)[None, :]
        ang = 2 * np.pi * ((m * n) % LONS) / LONS
        tabs.append(np.concatenate([np.cos(ang), -np.sin(ang)], axis=1))
    back = np.stack(tabs)
    scale = np.full((2, 1, WAVES), 2.0 / LONS)
    scale[0, 0, 0] = 1.0 / LONS
    scale[0, 0, WAVES // 2] = 0.0

    def halves(x):
        x = x.astype(np.float32)
        hi = x.astype(jnp.bfloat16)
        return np.stack([hi, (x - hi.astype(np.float32)).astype(jnp.bfloat16)], axis=1)

    return halves(back * scale), halves(np.swapaxes(back, 1, 2))


ANY = pl.BlockSpec(memory_space=pl.ANY)
VM = pl.BlockSpec(memory_space=pltpu.VMEM)
DMA = pltpu.SemaphoreType.DMA
LIMIT = 60 * 1024 * 1024


def solution(mesh):
    dft, dft_t = dft_tables()

    def per_device(coef, legendre, gauss_weight):
        me = lax.axis_index('w')
        own = lax.dynamic_slice_in_dim(gauss_weight, me * LAT, LAT, axis=0)
        weight = jnp.tile(own, QQ)[None, :]
        _, grid_mid, spec_mid, last = pl.pallas_call(
            transform,
            out_shape=(
                jax.ShapeDtypeStruct((KK, 2, WAVES, LANES), F32),
                jax.ShapeDtypeStruct((LEVS, LAT, LONS), F32),
                jax.ShapeDtypeStruct((EARLY_WAVES, 2, LEVS, WAVES), F32),
                jax.ShapeDtypeStruct((DEVS, KK, 2, CHUNK, LANES), F32),
            ),
            in_specs=[ANY, ANY, VM, VM, VM],
            out_specs=(ANY, ANY, ANY, ANY),
            scratch_shapes=[
                pltpu.VMEM((NB, 2, LEVS, WAVES), F32),
                pltpu.VMEM((NB, WAVES, LATS), F32),
                pltpu.VMEM((2, WAVES, LANES), F32),
                pltpu.VMEM((2, LANES, LONS), F32),
                pltpu.VMEM((KK, 2, WAVES, LANES), F32),
                pltpu.VMEM((DEVS, 2, KK, 2, OWN // 2, LANES), F32),
                pltpu.VMEM((2, 2, LEVS, WAVES), F32),
                DMA((NB,)), DMA((NB,)), DMA, DMA((2, QQ)), DMA((2,)),
                DMA((DEVS,)), DMA((DEVS,)), DMA((KK, DEVS)), DMA((KK, DEVS)), DMA((DEVS,)), DMA((DEVS,)), DMA((CHUNKS, DEVS)),
            ],
            compiler_params=pltpu.CompilerParams(collective_id=0, has_side_effects=True, vmem_limit_bytes=LIMIT),
            name='transform',
        )(coef, legendre, dft, dft_t, weight)
        grid, spec_out = pl.pallas_call(
            finish,
            out_shape=(jax.ShapeDtypeStruct((LEVS, LAT, LONS), F32), jax.ShapeDtypeStruct((OWN, 2, LEVS, WAVES), F32)),
            in_specs=[ANY, ANY, ANY, ANY],
            out_specs=(ANY, ANY),
            scratch_shapes=[
                pltpu.VMEM((DEVS, KK, 2, CHUNK, LANES), F32),
                pltpu.VMEM((CHUNK, WAVES, LATS), F32),
                pltpu.VMEM((CHUNK, 2, LEVS, WAVES), F32),
                pltpu.VMEM((CHUNK, QQ, LAT, LONS), F32),
                pltpu.VMEM((EARLY_WAVES, 2, LEVS, WAVES), F32),
                DMA, DMA((CHUNK,)), DMA((CHUNK,)), DMA((2, CHUNK)), DMA((CHUNK,)), DMA((EARLY_WAVES,)),
            ],
            compiler_params=pltpu.CompilerParams(vmem_limit_bytes=LIMIT),
            name='finish',
        )(last, legendre, grid_mid, spec_mid)
        return grid, spec_out

    return jax.shard_map(per_device, mesh=mesh, in_specs=(P('w', None, 'lev', None), P(None, None, None), P(None)), out_specs=(P('lev', 'w', None), P('w', None, 'lev', None)), check_vma=False)
```

```python
import functools

import jax
import jax.numpy as jnp
import numpy as np
from jax import lax
from jax.experimental import pallas as pl
from jax.experimental.pallas import tpu as pltpu
from jax.sharding import PartitionSpec as P

DEVS = 8
WAVES = 512
OWN = WAVES // DEVS
LATS = 768
LAT = LATS // DEVS
LEVS = 32
LONS = 1024
HALF = LONS // 2
KK = 8
QQ = 4
LANES = QQ * LAT
CHUNK = 8
NB = 5
CHUNKS = OWN // CHUNK
FIRST = 6
EARLY = 2
AHEAD = 3
EARLY_WAVES = OWN - CHUNK
BF = jnp.bfloat16
F32 = jnp.float32


def split(x):
    hi = x.astype(BF)
    return hi, (x - hi.astype(F32)).astype(BF)


def dot3(a_hi, a_lo, b_hi, b_lo, dims):
    mm = functools.partial(lax.dot_general, dimension_numbers=(dims, ((), ())), preferred_element_type=F32)
    return mm(a_hi, b_hi) + (mm(a_hi, b_lo) + mm(a_lo, b_hi))


def dot_stacked(a, b, dims):
    rows = a.shape[0]
    (a_hi, a_lo), (b_hi, b_lo) = split(a), split(b)
    mm = functools.partial(lax.dot_general, dimension_numbers=(dims, ((), ())), preferred_element_type=F32)
    both = mm(jnp.concatenate([a_hi, a_lo], axis=0), b_hi)
    return both[:rows] + (both[rows:] + mm(a_hi, b_lo))


def barrier_all(me):
    sem = pltpu.get_barrier_semaphore()
    for o in range(1, DEVS):
        pl.semaphore_signal(sem, inc=1, device_id={'w': lax.rem(me + o, DEVS)}, device_id_type=pl.DeviceIdType.MESH)
    pl.semaphore_wait(sem, DEVS - 1)


def own_wave(t):
    return 2 * lax.rem(t, OWN // 2) + lax.div(t, OWN // 2)


def gather_rows(hbuf, i):
    rows = []
    for r in range(2):
        parts = [jnp.concatenate([hbuf[d, kk, r, pl.ds(i, 1), :] for kk in range(KK)], axis=0) for d in range(DEVS)]
        for q in range(QQ):
            rows.append(jnp.concatenate([p[:, q * LAT:(q + 1) * LAT] for p in parts], axis=1))
    return jnp.concatenate(rows, axis=0)


def transform(coef, leg, dft, dft_t, weight, frecv, grid_out, spec_out, last_out, cbuf, lbuf, fbuf, both, hrecv, csem, lsem, fsem, fs1, fr1, fs2, fr2, ssem, asem, bsem):
    me = lax.axis_index('w')
    barrier_all(me)

    def fetch_leg(t):
        slot = lax.rem(t, NB)
        return pltpu.make_async_copy(leg.at[me * OWN + own_wave(t)], lbuf.at[slot], lsem.at[slot])

    def fetch_coef(t):
        slot = lax.rem(t, NB)
        return pltpu.make_async_copy(coef.at[own_wave(t)], cbuf.at[slot], csem.at[slot])

    def target(o):
        return lax.rem(me + o, DEVS)

    def source(o):
        return lax.rem(me - o + DEVS, DEVS)

    def block(d, row=0, size=OWN):
        return pl.ds(pl.multiple_of(d * OWN + row, CHUNK), size)

    def move(o, src_ref, dst_ref, send_sem, recv_sem):
        if o == 0:
            pltpu.make_async_copy(src_ref, dst_ref, recv_sem).start()
        else:
            pltpu.make_async_remote_copy(src_ref=src_ref, dst_ref=dst_ref, send_sem=send_sem, recv_sem=recv_sem, device_id={'w': target(o)}, device_id_type=pl.DeviceIdType.MESH).start()

    def wait_for(part, sem):
        pltpu.make_async_copy(part, part, sem).wait()

    for t in range(NB):
        fetch_leg(t).start()
        fetch_coef(t).start()

    @pl.loop(0, CHUNKS)
    def _(c):
        @pl.loop(0, CHUNK)
        def _(i):
            t = c * CHUNK + i
            fetch_leg(t).wait()
            fetch_coef(t).wait()
            buf = lax.rem(t, NB)
            f = dot_stacked(cbuf[buf].reshape(2 * LEVS, WAVES), lbuf[buf], ((1,), (0,)))

            @pl.when(t + NB < OWN)
            def _():
                fetch_leg(t + NB).start()
                fetch_coef(t + NB).start()

            for d in range(DEVS):
                cols = f[:, d * LAT:(d + 1) * LAT]
                for r in range(2):
                    row = r * LEVS
                    packed = jnp.concatenate([cols[row + q * KK:row + (q + 1) * KK] for q in range(QQ)], axis=1)
                    for kk in range(KK):
                        both[kk, r, pl.ds(d * OWN + t, 1), :] = packed[kk:kk + 1]

        for o in range(DEVS):
            move(o, both.at[pl.ds(0, FIRST), :, block(target(o), c * CHUNK, CHUNK), :], frecv.at[pl.ds(0, FIRST), :, block(me, c * CHUNK, CHUNK), :], fs1.at[o], fr1.at[o])

    for kk in range(FIRST, KK):
        for o in range(DEVS):
            move(o, both.at[kk, :, block(target(o)), :], frecv.at[kk, :, block(me), :], fs2.at[kk, o], fr2.at[kk, o])
    for t in range(NB):
        fetch_leg(t).start()

    def dst_rows(o, row, size):
        return pl.ds(pl.multiple_of(target(o) * (OWN // 2) + row, CHUNK), size)

    def send_levels(kk):
        for o in range(DEVS):
            for par in range(2):
                move(o, both.at[kk, :, dst_rows(o, par * (WAVES // 2), OWN // 2), :], hrecv.at[me, par, kk], ssem.at[o], asem.at[o])

    def chunk_at(ref, c):
        row = pl.multiple_of(lax.rem(c, 4) * CHUNK, CHUNK)
        return ref.at[lax.div(c, 4), pl.ds(EARLY, KK - EARLY), :, pl.ds(row, CHUNK), :]

    def send_chunk(c):
        row = lax.div(c, 4) * (WAVES // 2) + lax.rem(c, 4) * CHUNK
        for o in range(DEVS):
            move(o, both.at[pl.ds(EARLY, KK - EARLY), :, dst_rows(o, row, CHUNK), :], chunk_at(hrecv.at[me], c), ssem.at[o], bsem.at[c, o])

    def arrived(c):
        for o in range(DEVS):
            wait_for(chunk_at(hrecv.at[source(o)], c), bsem.at[c, o])

    @pl.loop(0, KK)
    def _(kk):
        @pl.when(kk == 0)
        def _():
            for o in range(DEVS):
                wait_for(frecv.at[pl.ds(0, FIRST), :, block(source(o)), :], fr1.at[o])
            for o in range(1, DEVS):
                wait_for(both.at[pl.ds(0, FIRST), :, block(target(o)), :], fs1.at[o])

        @pl.when(kk >= FIRST)
        def _():
            for o in range(DEVS):
                wait_for(frecv.at[kk, :, block(source(o)), :], fr2.at[kk, o])
            for o in range(1, DEVS):
                wait_for(both.at[kk, :, block(target(o)), :], fs2.at[kk, o])

        fetch = pltpu.make_async_copy(frecv.at[kk], fbuf, fsem)
        fetch.start()
        fetch.wait()

        sums = []
        for par in range(2):
            x = jnp.concatenate([fbuf[r, d * OWN + par * (OWN // 2):d * OWN + (par + 1) * (OWN // 2), :] for r in range(2) for d in range(DEVS)], axis=0)
            x_hi, x_lo = split(x)
            sums.append(dot3(dft[par, 0], dft[par, 1], x_hi, x_lo, ((1,), (0,))))
        first, second = sums[0] + sums[1], sums[0] - sums[1]
        for half, y in enumerate((first.T, second.T)):
            for q in range(QQ):
                grid_out[q * KK + kk, :, half * HALF:(half + 1) * HALF] = y[q * LAT:(q + 1) * LAT]
        first, second = first * first, second * second
        for par, y in enumerate((first + second, first - second)):
            y_hi, y_lo = split(y)
            h = dot3(dft_t[par, 0], dft_t[par, 1], y_hi, y_lo, ((1,), (0,))) * weight[...]
            for r in range(2):
                both[kk, r, par * (WAVES // 2):(par + 1) * (WAVES // 2), :] = h[r * (WAVES // 2):(r + 1) * (WAVES // 2)]

        @pl.when(kk < EARLY)
        def _():
            send_levels(kk)

    for c in range(AHEAD):
        send_chunk(c)
    for o in range(DEVS):
        wait_for(hrecv.at[source(o), :, pl.ds(0, EARLY)], asem.at[o])

    @pl.loop(0, CHUNKS - 1)
    def _(c):
        arrived(c)

        @pl.when(c + AHEAD < CHUNKS)
        def _():
            send_chunk(c + AHEAD)

        par, row = lax.div(c, 4), lax.rem(c, 4) * CHUNK

        @pl.loop(0, CHUNK)
        def _(i):
            t = c * CHUNK + i
            h = gather_rows(hrecv.at[:, par], row + i)
            fetch_leg(t).wait()

            spec_out[t] = dot_stacked(h, lbuf[lax.rem(t, NB)], ((1,), (1,))).reshape(2, LEVS, WAVES)

            @pl.when(t + NB < EARLY_WAVES)
            def _():
                fetch_leg(t + NB).start()

    arrived(CHUNKS - 1)
    last_out[...] = hrecv[:, 1, :, :, 3 * CHUNK:4 * CHUNK, :]
    for o in range(1, DEVS):
        wait_for(both.at[:, :, block(target(o)), :], ssem.at[o])


def finish(h_in, leg, grid_in, spec_in, grid_out, spec_out, lbuf, obuf, lsem, osem, gsem, ssem):
    me = lax.axis_index('w')

    def fetch_leg(i):
        return pltpu.make_async_copy(leg.at[me * OWN + own_wave(EARLY_WAVES + i)], lbuf.at[i], lsem.at[i])

    def grid_copy(i):
        return pltpu.make_async_copy(grid_in.at[pl.ds(i * QQ, QQ)], grid_out.at[pl.ds(i * QQ, QQ)], gsem.at[i])

    def spec_copy(t):
        return pltpu.make_async_copy(spec_in.at[t], spec_out.at[own_wave(t)], ssem.at[t])

    def store(i):
        return pltpu.make_async_copy(obuf.at[i], spec_out.at[own_wave(EARLY_WAVES + i)], osem.at[i])

    for i in range(CHUNK):
        fetch_leg(i).start()
    for i in range(CHUNK):
        grid_copy(i).start()

    @pl.loop(0, EARLY_WAVES)
    def _(t):
        spec_copy(t).start()

    @pl.loop(0, CHUNK)
    def _(i):
        h = gather_rows(h_in, i)
        fetch_leg(i).wait()
        obuf[i] = dot_stacked(h, lbuf[i], ((1,), (1,))).reshape(2, LEVS, WAVES)
        store(i).start()

    @pl.loop(0, CHUNK)
    def _(i):
        store(i).wait()
        grid_copy(i).wait()

    @pl.loop(0, EARLY_WAVES)
    def _(t):
        spec_copy(t).wait()


def dft_tables():
    n = np.arange(HALF)[:, None]
    tabs = []
    for par in range(2):
        m = np.arange(par, WAVES, 2)[None, :]
        ang = 2 * np.pi * ((m * n) % LONS) / LONS
        tabs.append(np.concatenate([np.cos(ang), -np.sin(ang)], axis=1))
    back = np.stack(tabs)
    scale = np.full((2, 1, WAVES), 2.0 / LONS)
    scale[0, 0, 0] = 1.0 / LONS
    scale[0, 0, WAVES // 2] = 0.0

    def halves(x):
        x = x.astype(np.float32)
        hi = x.astype(jnp.bfloat16)
        return np.stack([hi, (x - hi.astype(np.float32)).astype(jnp.bfloat16)], axis=1)

    return halves(back * scale), halves(np.swapaxes(back, 1, 2))


ANY = pl.BlockSpec(memory_space=pl.ANY)
VM = pl.BlockSpec(memory_space=pltpu.VMEM)
DMA = pltpu.SemaphoreType.DMA
LIMIT = 42 * 1024 * 1024
LIMIT_END = 18 * 1024 * 1024


def solution(mesh):
    dft, dft_t = dft_tables()

    def per_device(coef, legendre, gauss_weight):
        me = lax.axis_index('w')
        own = lax.dynamic_slice_in_dim(gauss_weight, me * LAT, LAT, axis=0)
        weight = jnp.tile(own, QQ)[None, :]
        _, grid_mid, spec_mid, last = pl.pallas_call(
            transform,
            out_shape=(
                jax.ShapeDtypeStruct((KK, 2, WAVES, LANES), F32),
                pltpu.VMEM((LEVS, LAT, LONS), F32),
                pltpu.VMEM((EARLY_WAVES, 2, LEVS, WAVES), F32),
                pltpu.VMEM((DEVS, KK, 2, CHUNK, LANES), F32),
            ),
            in_specs=[ANY, ANY, VM, VM, VM],
            out_specs=(ANY, VM, VM, VM),
            scratch_shapes=[
                pltpu.VMEM((NB, 2, LEVS, WAVES), F32),
                pltpu.VMEM((NB, WAVES, LATS), F32),
                pltpu.VMEM((2, WAVES, LANES), F32),
                pltpu.VMEM((KK, 2, WAVES, LANES), F32),
                pltpu.VMEM((DEVS, 2, KK, 2, OWN // 2, LANES), F32),
                DMA((NB,)), DMA((NB,)), DMA,
                DMA((DEVS,)), DMA((DEVS,)), DMA((KK, DEVS)), DMA((KK, DEVS)), DMA((DEVS,)), DMA((DEVS,)), DMA((CHUNKS, DEVS)),
            ],
            compiler_params=pltpu.CompilerParams(collective_id=0, has_side_effects=True, vmem_limit_bytes=LIMIT),
            name='transform',
        )(coef, legendre, dft, dft_t, weight)
        grid, spec_out = pl.pallas_call(
            finish,
            out_shape=(jax.ShapeDtypeStruct((LEVS, LAT, LONS), F32), jax.ShapeDtypeStruct((OWN, 2, LEVS, WAVES), F32)),
            in_specs=[VM, ANY, ANY, ANY],
            out_specs=(ANY, ANY),
            scratch_shapes=[
                pltpu.VMEM((CHUNK, WAVES, LATS), F32),
                pltpu.VMEM((CHUNK, 2, LEVS, WAVES), F32),
                DMA((CHUNK,)), DMA((CHUNK,)), DMA((CHUNK,)), DMA((EARLY_WAVES,)),
            ],
            compiler_params=pltpu.CompilerParams(vmem_limit_bytes=LIMIT_END),
            name='finish',
        )(last, legendre, grid_mid, spec_mid)
        return grid, spec_out

    return jax.shard_map(per_device, mesh=mesh, in_specs=(P('w', None, 'lev', None), P(None, None, None), P(None)), out_specs=(P('lev', 'w', None), P('w', None, 'lev', None)), check_vma=False)
```

```python
import functools

import jax
import jax.numpy as jnp
import numpy as np
from jax import lax
from jax.experimental import pallas as pl
from jax.experimental.pallas import tpu as pltpu
from jax.sharding import PartitionSpec as P

DEVS = 8
WAVES = 512
OWN = WAVES // DEVS
LATS = 768
LAT = LATS // DEVS
LEVS = 32
LONS = 1024
HALF = LONS // 2
KK = 8
QQ = 4
LANES = QQ * LAT
CHUNK = 8
NB = 5
CHUNKS = OWN // CHUNK
FIRST = 6
EARLY = 2
AHEAD = 3
EARLY_WAVES = OWN - CHUNK
BF = jnp.bfloat16
F32 = jnp.float32


def split(x):
    hi = x.astype(BF)
    return hi, (x - hi.astype(F32)).astype(BF)


def dot3(a_hi, a_lo, b_hi, b_lo, dims):
    mm = functools.partial(lax.dot_general, dimension_numbers=(dims, ((), ())), preferred_element_type=F32)
    return mm(a_hi, b_hi) + (mm(a_hi, b_lo) + mm(a_lo, b_hi))


def dot_stacked(a, b, dims):
    rows = a.shape[0]
    (a_hi, a_lo), (b_hi, b_lo) = split(a), split(b)
    mm = functools.partial(lax.dot_general, dimension_numbers=(dims, ((), ())), preferred_element_type=F32)
    both = mm(jnp.concatenate([a_hi, a_lo], axis=0), b_hi)
    return both[:rows] + (both[rows:] + mm(a_hi, b_lo))


def barrier_signal(me):
    sem = pltpu.get_barrier_semaphore()
    for o in range(1, DEVS):
        pl.semaphore_signal(sem, inc=1, device_id={'w': lax.rem(me + o, DEVS)}, device_id_type=pl.DeviceIdType.MESH)


def barrier_wait():
    pl.semaphore_wait(pltpu.get_barrier_semaphore(), DEVS - 1)


def own_wave(t):
    return 2 * lax.rem(t, OWN // 2) + lax.div(t, OWN // 2)


def gather_rows(hbuf, i):
    rows = []
    for r in range(2):
        parts = [jnp.concatenate([hbuf[d, kk, r, pl.ds(i, 1), :] for kk in range(KK)], axis=0) for d in range(DEVS)]
        for q in range(QQ):
            rows.append(jnp.concatenate([p[:, q * LAT:(q + 1) * LAT] for p in parts], axis=1))
    return jnp.concatenate(rows, axis=0)


def transform(coef, leg, dft, dft_t, weight, frecv, grid_out, spec_out, last_out, cbuf, lbuf, fbuf, both, hrecv, csem, lsem, fsem, fs1, fr1, fs2, fr2, ssem, asem, bsem):
    me = lax.axis_index('w')
    barrier_signal(me)

    def fetch_leg(t):
        slot = lax.rem(t, NB)
        return pltpu.make_async_copy(leg.at[me * OWN + own_wave(t)], lbuf.at[slot], lsem.at[slot])

    def fetch_coef(t):
        slot = lax.rem(t, NB)
        return pltpu.make_async_copy(coef.at[own_wave(t)], cbuf.at[slot], csem.at[slot])

    def target(o):
        return lax.rem(me + o, DEVS)

    def source(o):
        return lax.rem(me - o + DEVS, DEVS)

    def block(d, row=0, size=OWN):
        return pl.ds(pl.multiple_of(d * OWN + row, CHUNK), size)

    def move(o, src_ref, dst_ref, send_sem, recv_sem):
        if o == 0:
            pltpu.make_async_copy(src_ref, dst_ref, recv_sem).start()
        else:
            pltpu.make_async_remote_copy(src_ref=src_ref, dst_ref=dst_ref, send_sem=send_sem, recv_sem=recv_sem, device_id={'w': target(o)}, device_id_type=pl.DeviceIdType.MESH).start()

    own_weight = weight[:, 0:LAT]
    for d in range(1, DEVS):
        own_weight = jnp.where(me == d, weight[:, d * LAT:(d + 1) * LAT], own_weight)
    own_weight = jnp.concatenate([own_weight] * QQ, axis=1)

    def wait_for(part, sem):
        pltpu.make_async_copy(part, part, sem).wait()

    for t in range(NB):
        fetch_leg(t).start()
        fetch_coef(t).start()

    @pl.loop(0, CHUNKS)
    def _(c):
        @pl.loop(0, CHUNK)
        def _(i):
            t = c * CHUNK + i
            fetch_leg(t).wait()
            fetch_coef(t).wait()
            buf = lax.rem(t, NB)
            f = dot_stacked(cbuf[buf].reshape(2 * LEVS, WAVES), lbuf[buf], ((1,), (0,)))

            @pl.when(t + NB < OWN)
            def _():
                fetch_leg(t + NB).start()
                fetch_coef(t + NB).start()

            for d in range(DEVS):
                cols = f[:, d * LAT:(d + 1) * LAT]
                for r in range(2):
                    row = r * LEVS
                    packed = jnp.concatenate([cols[row + q * KK:row + (q + 1) * KK] for q in range(QQ)], axis=1)
                    for kk in range(KK):
                        both[kk, r, pl.ds(d * OWN + t, 1), :] = packed[kk:kk + 1]

        @pl.when(c == 0)
        def _():
            barrier_wait()

        for o in range(DEVS):
            move(o, both.at[pl.ds(0, FIRST), :, block(target(o), c * CHUNK, CHUNK), :], frecv.at[pl.ds(0, FIRST), :, block(me, c * CHUNK, CHUNK), :], fs1.at[o], fr1.at[o])

    for kk in range(FIRST, KK):
        for o in range(DEVS):
            move(o, both.at[kk, :, block(target(o)), :], frecv.at[kk, :, block(me), :], fs2.at[kk, o], fr2.at[kk, o])
    for t in range(NB):
        fetch_leg(t).start()

    def dst_rows(o, row, size):
        return pl.ds(pl.multiple_of(target(o) * (OWN // 2) + row, CHUNK), size)

    def send_levels(kk):
        for o in range(DEVS):
            for par in range(2):
                move(o, both.at[kk, :, dst_rows(o, par * (WAVES // 2), OWN // 2), :], hrecv.at[me, par, kk], ssem.at[o], asem.at[o])

    def chunk_at(ref, c):
        row = pl.multiple_of(lax.rem(c, 4) * CHUNK, CHUNK)
        return ref.at[lax.div(c, 4), pl.ds(EARLY, KK - EARLY), :, pl.ds(row, CHUNK), :]

    def send_chunk(c):
        row = lax.div(c, 4) * (WAVES // 2) + lax.rem(c, 4) * CHUNK
        for o in range(DEVS):
            move(o, both.at[pl.ds(EARLY, KK - EARLY), :, dst_rows(o, row, CHUNK), :], chunk_at(hrecv.at[me], c), ssem.at[o], bsem.at[c, o])

    def arrived(c):
        for o in range(DEVS):
            wait_for(chunk_at(hrecv.at[source(o)], c), bsem.at[c, o])

    @pl.loop(0, KK)
    def _(kk):
        @pl.when(kk == 0)
        def _():
            for o in range(DEVS):
                wait_for(frecv.at[pl.ds(0, FIRST), :, block(source(o)), :], fr1.at[o])
            for o in range(1, DEVS):
                wait_for(both.at[pl.ds(0, FIRST), :, block(target(o)), :], fs1.at[o])

        @pl.when(kk >= FIRST)
        def _():
            for o in range(DEVS):
                wait_for(frecv.at[kk, :, block(source(o)), :], fr2.at[kk, o])
            for o in range(1, DEVS):
                wait_for(both.at[kk, :, block(target(o)), :], fs2.at[kk, o])

        fetch = pltpu.make_async_copy(frecv.at[kk], fbuf, fsem)
        fetch.start()
        fetch.wait()

        sums = []
        for par in range(2):
            x = jnp.concatenate([fbuf[r, d * OWN + par * (OWN // 2):d * OWN + (par + 1) * (OWN // 2), :] for r in range(2) for d in range(DEVS)], axis=0)
            x_hi, x_lo = split(x)
            sums.append(dot3(dft[par, 0], dft[par, 1], x_hi, x_lo, ((1,), (0,))))
        first, second = sums[0] + sums[1], sums[0] - sums[1]
        for half, y in enumerate((first.T, second.T)):
            for q in range(QQ):
                grid_out[q * KK + kk, :, half * HALF:(half + 1) * HALF] = y[q * LAT:(q + 1) * LAT]
        first, second = first * first, second * second
        for par, y in enumerate((first + second, first - second)):
            y_hi, y_lo = split(y)
            h = dot3(dft_t[par, 0], dft_t[par, 1], y_hi, y_lo, ((1,), (0,))) * own_weight
            for r in range(2):
                both[kk, r, par * (WAVES // 2):(par + 1) * (WAVES // 2), :] = h[r * (WAVES // 2):(r + 1) * (WAVES // 2)]

        @pl.when(kk < EARLY)
        def _():
            send_levels(kk)

    for c in range(AHEAD):
        send_chunk(c)
    for o in range(DEVS):
        wait_for(hrecv.at[source(o), :, pl.ds(0, EARLY)], asem.at[o])

    @pl.loop(0, CHUNKS - 1)
    def _(c):
        arrived(c)

        @pl.when(c + AHEAD < CHUNKS)
        def _():
            send_chunk(c + AHEAD)

        par, row = lax.div(c, 4), lax.rem(c, 4) * CHUNK

        @pl.loop(0, CHUNK)
        def _(i):
            t = c * CHUNK + i
            h = gather_rows(hrecv.at[:, par], row + i)
            fetch_leg(t).wait()

            spec_out[t] = dot_stacked(h, lbuf[lax.rem(t, NB)], ((1,), (1,))).reshape(2, LEVS, WAVES)

            @pl.when(t + NB < EARLY_WAVES)
            def _():
                fetch_leg(t + NB).start()

    arrived(CHUNKS - 1)
    last_out[...] = hrecv[:, 1, :, :, 3 * CHUNK:4 * CHUNK, :]
    for o in range(1, DEVS):
        wait_for(both.at[:, :, block(target(o)), :], ssem.at[o])


def finish(h_in, leg, grid_in, spec_in, grid_out, spec_out, lbuf, obuf, lsem, osem, gsem, ssem):
    me = lax.axis_index('w')

    def fetch_leg(i):
        return pltpu.make_async_copy(leg.at[me * OWN + own_wave(EARLY_WAVES + i)], lbuf.at[i], lsem.at[i])

    def grid_copy(i):
        return pltpu.make_async_copy(grid_in.at[pl.ds(i * QQ, QQ)], grid_out.at[pl.ds(i * QQ, QQ)], gsem.at[i])

    def spec_copy(t):
        return pltpu.make_async_copy(spec_in.at[t], spec_out.at[own_wave(t)], ssem.at[t])

    def store(i):
        return pltpu.make_async_copy(obuf.at[i], spec_out.at[own_wave(EARLY_WAVES + i)], osem.at[i])

    for i in range(CHUNK):
        fetch_leg(i).start()
    for i in range(CHUNK):
        grid_copy(i).start()

    @pl.loop(0, EARLY_WAVES)
    def _(t):
        spec_copy(t).start()

    @pl.loop(0, CHUNK)
    def _(i):
        h = gather_rows(h_in, i)
        fetch_leg(i).wait()
        obuf[i] = dot_stacked(h, lbuf[i], ((1,), (1,))).reshape(2, LEVS, WAVES)
        store(i).start()

    @pl.loop(0, CHUNK)
    def _(i):
        store(i).wait()
        grid_copy(i).wait()

    @pl.loop(0, EARLY_WAVES)
    def _(t):
        spec_copy(t).wait()


def dft_tables():
    n = np.arange(HALF)[:, None]
    tabs = []
    for par in range(2):
        m = np.arange(par, WAVES, 2)[None, :]
        ang = 2 * np.pi * ((m * n) % LONS) / LONS
        tabs.append(np.concatenate([np.cos(ang), -np.sin(ang)], axis=1))
    back = np.stack(tabs)
    scale = np.full((2, 1, WAVES), 2.0 / LONS)
    scale[0, 0, 0] = 1.0 / LONS
    scale[0, 0, WAVES // 2] = 0.0

    def halves(x):
        x = x.astype(np.float32)
        hi = x.astype(jnp.bfloat16)
        return np.stack([hi, (x - hi.astype(np.float32)).astype(jnp.bfloat16)], axis=1)

    return halves(back * scale), halves(np.swapaxes(back, 1, 2))


ANY = pl.BlockSpec(memory_space=pl.ANY)
VM = pl.BlockSpec(memory_space=pltpu.VMEM)
DMA = pltpu.SemaphoreType.DMA
LIMIT = 42 * 1024 * 1024
LIMIT_END = 18 * 1024 * 1024


def solution(mesh):
    dft, dft_t = dft_tables()

    def per_device(coef, legendre, gauss_weight):
        _, grid_mid, spec_mid, last = pl.pallas_call(
            transform,
            out_shape=(
                jax.ShapeDtypeStruct((KK, 2, WAVES, LANES), F32),
                pltpu.VMEM((LEVS, LAT, LONS), F32),
                pltpu.VMEM((EARLY_WAVES, 2, LEVS, WAVES), F32),
                pltpu.VMEM((DEVS, KK, 2, CHUNK, LANES), F32),
            ),
            in_specs=[ANY, ANY, VM, VM, VM],
            out_specs=(ANY, VM, VM, VM),
            scratch_shapes=[
                pltpu.VMEM((NB, 2, LEVS, WAVES), F32),
                pltpu.VMEM((NB, WAVES, LATS), F32),
                pltpu.VMEM((2, WAVES, LANES), F32),
                pltpu.VMEM((KK, 2, WAVES, LANES), F32),
                pltpu.VMEM((DEVS, 2, KK, 2, OWN // 2, LANES), F32),
                DMA((NB,)), DMA((NB,)), DMA,
                DMA((DEVS,)), DMA((DEVS,)), DMA((KK, DEVS)), DMA((KK, DEVS)), DMA((DEVS,)), DMA((DEVS,)), DMA((CHUNKS, DEVS)),
            ],
            compiler_params=pltpu.CompilerParams(collective_id=0, has_side_effects=True, vmem_limit_bytes=LIMIT),
            name='transform',
        )(coef, legendre, dft, dft_t, gauss_weight[None, :])
        grid, spec_out = pl.pallas_call(
            finish,
            out_shape=(jax.ShapeDtypeStruct((LEVS, LAT, LONS), F32), jax.ShapeDtypeStruct((OWN, 2, LEVS, WAVES), F32)),
            in_specs=[VM, ANY, ANY, ANY],
            out_specs=(ANY, ANY),
            scratch_shapes=[
                pltpu.VMEM((CHUNK, WAVES, LATS), F32),
                pltpu.VMEM((CHUNK, 2, LEVS, WAVES), F32),
                DMA((CHUNK,)), DMA((CHUNK,)), DMA((CHUNK,)), DMA((EARLY_WAVES,)),
            ],
            compiler_params=pltpu.CompilerParams(vmem_limit_bytes=LIMIT_END),
            name='finish',
        )(last, legendre, grid_mid, spec_mid)
        return grid, spec_out

    return jax.shard_map(per_device, mesh=mesh, in_specs=(P('w', None, 'lev', None), P(None, None, None), P(None)), out_specs=(P('lev', 'w', None), P('w', None, 'lev', None)), check_vma=False)
```

```python
import functools

import jax
import jax.numpy as jnp
import numpy as np
from jax import lax
from jax.experimental import pallas as pl
from jax.experimental.pallas import tpu as pltpu
from jax.sharding import PartitionSpec as P

DEVS = 8
WAVES = 512
OWN = WAVES // DEVS
LATS = 768
LAT = LATS // DEVS
LEVS = 32
LONS = 1024
HALF = LONS // 2
KK = 8
QQ = 4
SIDE = 4
LANES = QQ * LAT
CHUNK = 8
NB = 5
CHUNKS = OWN // CHUNK
FIRST = 6
EARLY = 2
AHEAD = 3
EARLY_WAVES = OWN - CHUNK
BF = jnp.bfloat16
F32 = jnp.float32


def split(x):
    hi = x.astype(BF)
    return hi, (x - hi.astype(F32)).astype(BF)


def dot3(a_hi, a_lo, b_hi, b_lo, dims):
    mm = functools.partial(lax.dot_general, dimension_numbers=(dims, ((), ())), preferred_element_type=F32)
    return mm(a_hi, b_hi) + (mm(a_hi, b_lo) + mm(a_lo, b_hi))


def dot_stacked(a, b, dims):
    rows = a.shape[0]
    (a_hi, a_lo), (b_hi, b_lo) = split(a), split(b)
    mm = functools.partial(lax.dot_general, dimension_numbers=(dims, ((), ())), preferred_element_type=F32)
    both = mm(jnp.concatenate([a_hi, a_lo], axis=0), b_hi)
    return both[:rows] + (both[rows:] + mm(a_hi, b_lo))


def barrier_signal(me):
    sem = pltpu.get_barrier_semaphore()
    for o in range(1, DEVS):
        pl.semaphore_signal(sem, inc=1, device_id={'w': lax.rem(me + o, DEVS)}, device_id_type=pl.DeviceIdType.MESH)


def barrier_wait():
    pl.semaphore_wait(pltpu.get_barrier_semaphore(), DEVS - 1)


def own_wave(t):
    return 2 * lax.rem(t, OWN // 2) + lax.div(t, OWN // 2)


def gather_rows(hbuf, i):
    rows = []
    for r in range(2):
        parts = [jnp.concatenate([hbuf[d, kk, r, pl.ds(i, 1), :] for kk in range(KK)], axis=0) for d in range(DEVS)]
        for q in range(QQ):
            rows.append(jnp.concatenate([p[:, q * LAT:(q + 1) * LAT] for p in parts], axis=1))
    return jnp.concatenate(rows, axis=0)


def whole(lbuf, slot):
    return jnp.concatenate([lbuf[slot, 0], lbuf[slot, 1]], axis=1)


def transform(coef, leg, dft, dft_t, weight, frecv, spec_out, last_out, lbuf, grid_out, cbuf, fbuf, both, hrecv, csem, hsem, lsem, fsem, fs1, fr1, fs2, fr2, ssem, asem, bsem):
    me = lax.axis_index('w')
    barrier_signal(me)

    row, col = lax.div(me, SIDE), lax.rem(me, SIDE)

    def fetch_half(u):
        t = lax.div(u, 2 * CHUNK) * CHUNK + lax.rem(u, CHUNK)
        side = lax.rem(row + 1 + lax.rem(lax.div(u, CHUNK), 2), 2)
        cols = pl.ds(pl.multiple_of(side * LANES, LANES), LANES)
        buf = lax.rem(u, 2 * NB)
        return pltpu.make_async_copy(leg.at[me * OWN + own_wave(t), :, cols], lbuf.at[lax.div(buf, 2), lax.rem(buf, 2)], hsem.at[buf])

    def fetch_coef(u):
        t = lax.div(u, 2 * CHUNK) * CHUNK + lax.rem(u, CHUNK)
        slot = lax.rem(u, NB)
        return pltpu.make_async_copy(coef.at[own_wave(t)], cbuf.at[slot], csem.at[slot])

    def fetch_leg(t, half):
        slot = lax.rem(t, NB)
        cols = pl.ds(half * LANES, LANES)
        return pltpu.make_async_copy(leg.at[me * OWN + own_wave(t), :, cols], lbuf.at[slot, half], lsem.at[slot, half])

    def row_of(o):
        return row if o < SIDE else 1 - row

    def target(o):
        return row_of(o) * SIDE + lax.rem(col + o, SIDE)

    def source(o):
        return row_of(o) * SIDE + lax.rem(col - o + DEVS, SIDE)

    def block(d, row=0, size=OWN):
        return pl.ds(pl.multiple_of(d * OWN + row, CHUNK), size)

    def move(o, src_ref, dst_ref, send_sem, recv_sem):
        if o == 0:
            pltpu.make_async_copy(src_ref, dst_ref, recv_sem).start()
        else:
            pltpu.make_async_remote_copy(src_ref=src_ref, dst_ref=dst_ref, send_sem=send_sem, recv_sem=recv_sem, device_id={'w': target(o)}, device_id_type=pl.DeviceIdType.MESH).start()

    weights = weight[...].reshape(1, LATS)
    own_weight = weights[:, 0:LAT]
    for d in range(1, DEVS):
        own_weight = jnp.where(me == d, weights[:, d * LAT:(d + 1) * LAT], own_weight)
    own_weight = jnp.concatenate([own_weight] * QQ, axis=1)

    def wait_for(part, sem):
        pltpu.make_async_copy(part, part, sem).wait()

    for u in range(2 * NB):
        fetch_half(u).start()
    for u in range(NB):
        fetch_coef(u).start()

    @pl.loop(0, CHUNKS)
    def _(c):
        for part in range(2):
            side = lax.rem(row + 1 + part, 2)

            @pl.loop(0, CHUNK)
            def _(i):
                u = (2 * c + part) * CHUNK + i
                t = c * CHUNK + i
                fetch_half(u).wait()
                fetch_coef(u).wait()
                buf = lax.rem(u, 2 * NB)
                f = dot_stacked(cbuf[lax.rem(u, NB)].reshape(2 * LEVS, WAVES), lbuf[lax.div(buf, 2), lax.rem(buf, 2)], ((1,), (0,)))

                @pl.when(u + 2 * NB < 2 * OWN)
                def _():
                    fetch_half(u + 2 * NB).start()

                @pl.when(u + NB < 2 * OWN)
                def _():
                    fetch_coef(u + NB).start()

                for j in range(SIDE):
                    cols = f[:, j * LAT:(j + 1) * LAT]
                    for r in range(2):
                        packed = jnp.concatenate([cols[r * LEVS + q * KK:r * LEVS + (q + 1) * KK] for q in range(QQ)], axis=1)
                        for kk in range(KK):
                            both[kk, r, pl.ds((side * SIDE + j) * OWN + t, 1), :] = packed[kk:kk + 1]

            if part == 0:
                @pl.when(c == 0)
                def _():
                    barrier_wait()

            for o in range(SIDE):
                o += SIDE * (1 - part)
                move(o, both.at[pl.ds(0, FIRST), :, block(target(o), c * CHUNK, CHUNK), :], frecv.at[pl.ds(0, FIRST), :, block(me, c * CHUNK, CHUNK), :], fs1.at[o], fr1.at[o])

    for kk in range(FIRST, KK):
        for o in range(DEVS):
            move(o, both.at[kk, :, block(target(o)), :], frecv.at[kk, :, block(me), :], fs2.at[kk, o], fr2.at[kk, o])
    for t in range(NB):
        for half in range(2):
            fetch_leg(t, half).start()

    def dst_rows(o, row, size):
        return pl.ds(pl.multiple_of(target(o) * (OWN // 2) + row, CHUNK), size)

    def send_levels(kk):
        for o in range(DEVS):
            for par in range(2):
                move(o, both.at[kk, :, dst_rows(o, par * (WAVES // 2), OWN // 2), :], hrecv.at[me, par, kk], ssem.at[o], asem.at[o])

    def chunk_at(ref, c):
        row = pl.multiple_of(lax.rem(c, 4) * CHUNK, CHUNK)
        return ref.at[lax.div(c, 4), pl.ds(EARLY, KK - EARLY), :, pl.ds(row, CHUNK), :]

    def send_chunk(c):
        row = lax.div(c, 4) * (WAVES // 2) + lax.rem(c, 4) * CHUNK
        for o in range(DEVS):
            move(o, both.at[pl.ds(EARLY, KK - EARLY), :, dst_rows(o, row, CHUNK), :], chunk_at(hrecv.at[me], c), ssem.at[o], bsem.at[c, o])

    def arrived(c):
        for o in range(DEVS):
            wait_for(chunk_at(hrecv.at[source(o)], c), bsem.at[c, o])

    @pl.loop(0, KK)
    def _(kk):
        @pl.when(kk == 0)
        def _():
            for o in range(DEVS):
                wait_for(frecv.at[pl.ds(0, FIRST), :, block(source(o)), :], fr1.at[o])
            for o in range(1, DEVS):
                wait_for(both.at[pl.ds(0, FIRST), :, block(target(o)), :], fs1.at[o])

        @pl.when(kk >= FIRST)
        def _():
            for o in range(DEVS):
                wait_for(frecv.at[kk, :, block(source(o)), :], fr2.at[kk, o])
            for o in range(1, DEVS):
                wait_for(both.at[kk, :, block(target(o)), :], fs2.at[kk, o])

        fetch = pltpu.make_async_copy(frecv.at[kk], fbuf, fsem)
        fetch.start()
        fetch.wait()

        sums = []
        for par in range(2):
            x = jnp.concatenate([fbuf[r, d * OWN + par * (OWN // 2):d * OWN + (par + 1) * (OWN // 2), :] for r in range(2) for d in range(DEVS)], axis=0)
            x_hi, x_lo = split(x)
            sums.append(dot3(dft[par, 0], dft[par, 1], x_hi, x_lo, ((1,), (0,))))
        first, second = sums[0] + sums[1], sums[0] - sums[1]
        for half, y in enumerate((first.T, second.T)):
            for q in range(QQ):
                grid_out[q * KK + kk, :, half * HALF:(half + 1) * HALF] = y[q * LAT:(q + 1) * LAT]
        first, second = first * first, second * second
        for par, y in enumerate((first + second, first - second)):
            y_hi, y_lo = split(y)
            h = dot3(dft_t[par, 0], dft_t[par, 1], y_hi, y_lo, ((1,), (0,))) * own_weight
            for r in range(2):
                both[kk, r, par * (WAVES // 2):(par + 1) * (WAVES // 2), :] = h[r * (WAVES // 2):(r + 1) * (WAVES // 2)]

        @pl.when(kk < EARLY)
        def _():
            send_levels(kk)

    for c in range(AHEAD):
        send_chunk(c)
    for o in range(DEVS):
        wait_for(hrecv.at[source(o), :, pl.ds(0, EARLY)], asem.at[o])

    @pl.loop(0, CHUNKS - 1)
    def _(c):
        arrived(c)

        @pl.when(c + AHEAD < CHUNKS)
        def _():
            send_chunk(c + AHEAD)

        par, row = lax.div(c, 4), lax.rem(c, 4) * CHUNK

        @pl.loop(0, CHUNK)
        def _(i):
            t = c * CHUNK + i
            h = gather_rows(hrecv.at[:, par], row + i)
            for half in range(2):
                fetch_leg(t, half).wait()
            spec_out[t] = dot_stacked(h, whole(lbuf, lax.rem(t, NB)), ((1,), (1,))).reshape(2, LEVS, WAVES)

            @pl.when(t + NB < OWN)
            def _():
                for half in range(2):
                    fetch_leg(t + NB, half).start()

    arrived(CHUNKS - 1)
    for t in range(EARLY_WAVES, EARLY_WAVES + NB):
        for half in range(2):
            fetch_leg(t, half).wait()
    last_out[...] = hrecv[:, 1, :, :, 3 * CHUNK:4 * CHUNK, :]
    for o in range(1, DEVS):
        wait_for(both.at[:, :, block(target(o)), :], ssem.at[o])


def finish(h_in, leg_in, leg, grid_in, spec_in, grid_out, spec_out, lbuf, obuf, lsem, osem, gsem, ssem):
    me = lax.axis_index('w')

    def fetch_leg(i):
        return pltpu.make_async_copy(leg.at[me * OWN + own_wave(EARLY_WAVES + i)], lbuf.at[i - NB], lsem.at[i - NB])

    def grid_copy(i):
        return pltpu.make_async_copy(grid_in.at[pl.ds(i * QQ, QQ)], grid_out.at[pl.ds(i * QQ, QQ)], gsem.at[i])

    def spec_copy(t):
        return pltpu.make_async_copy(spec_in.at[t], spec_out.at[own_wave(t)], ssem.at[t])

    def store(i):
        return pltpu.make_async_copy(obuf.at[i], spec_out.at[own_wave(EARLY_WAVES + i)], osem.at[i])

    for i in range(NB, CHUNK):
        fetch_leg(i).start()
    for i in range(CHUNK):
        grid_copy(i).start()

    @pl.loop(0, EARLY_WAVES)
    def _(t):
        spec_copy(t).start()

    @pl.loop(0, NB)
    def _(i):
        block = whole(leg_in, lax.rem(EARLY_WAVES + i, NB))
        obuf[i] = dot_stacked(gather_rows(h_in, i), block, ((1,), (1,))).reshape(2, LEVS, WAVES)
        store(i).start()

    @pl.loop(NB, CHUNK)
    def _(i):
        h = gather_rows(h_in, i)
        fetch_leg(i).wait()
        obuf[i] = dot_stacked(h, lbuf[i - NB], ((1,), (1,))).reshape(2, LEVS, WAVES)
        store(i).start()

    @pl.loop(0, CHUNK)
    def _(i):
        store(i).wait()
        grid_copy(i).wait()

    @pl.loop(0, EARLY_WAVES)
    def _(t):
        spec_copy(t).wait()


def dft_tables():
    n = np.arange(HALF)[:, None]
    tabs = []
    for par in range(2):
        m = np.arange(par, WAVES, 2)[None, :]
        ang = 2 * np.pi * ((m * n) % LONS) / LONS
        tabs.append(np.concatenate([np.cos(ang), -np.sin(ang)], axis=1))
    back = np.stack(tabs)
    scale = np.full((2, 1, WAVES), 2.0 / LONS)
    scale[0, 0, 0] = 1.0 / LONS
    scale[0, 0, WAVES // 2] = 0.0

    def halves(x):
        x = x.astype(np.float32)
        hi = x.astype(jnp.bfloat16)
        return np.stack([hi, (x - hi.astype(np.float32)).astype(jnp.bfloat16)], axis=1)

    return halves(back * scale), halves(np.swapaxes(back, 1, 2))


ANY = pl.BlockSpec(memory_space=pl.ANY)
VM = pl.BlockSpec(memory_space=pltpu.VMEM)
DMA = pltpu.SemaphoreType.DMA
LIMIT = 35 * 1024 * 1024
LIMIT_END = 18 * 1024 * 1024


def solution(mesh):
    dft, dft_t = dft_tables()

    def per_device(coef, legendre, gauss_weight):
        _, spec_mid, last, leg_last, grid_mid = pl.pallas_call(
            transform,
            out_shape=(
                jax.ShapeDtypeStruct((KK, 2, WAVES, LANES), F32),
                pltpu.VMEM((EARLY_WAVES, 2, LEVS, WAVES), F32),
                pltpu.VMEM((DEVS, KK, 2, CHUNK, LANES), F32),
                pltpu.VMEM((NB, 2, WAVES, LANES), F32),
                pltpu.VMEM((LEVS, LAT, LONS), F32),
            ),
            in_specs=[ANY, ANY, VM, VM, VM],
            out_specs=(ANY, VM, VM, VM, VM),
            scratch_shapes=[
                pltpu.VMEM((NB, 2, LEVS, WAVES), F32),
                pltpu.VMEM((2, WAVES, LANES), F32),
                pltpu.VMEM((KK, 2, WAVES, LANES), F32),
                pltpu.VMEM((DEVS, 2, KK, 2, OWN // 2, LANES), F32),
                DMA((NB,)), DMA((2 * NB,)), DMA((NB, 2)), DMA,
                DMA((DEVS,)), DMA((DEVS,)), DMA((KK, DEVS)), DMA((KK, DEVS)), DMA((DEVS,)), DMA((DEVS,)), DMA((CHUNKS, DEVS)),
            ],
            compiler_params=pltpu.CompilerParams(collective_id=0, has_side_effects=True, vmem_limit_bytes=LIMIT),
            name='transform',
        )(coef, legendre, dft, dft_t, gauss_weight)
        grid, spec_out = pl.pallas_call(
            finish,
            out_shape=(jax.ShapeDtypeStruct((LEVS, LAT, LONS), F32), jax.ShapeDtypeStruct((OWN, 2, LEVS, WAVES), F32)),
            in_specs=[VM, VM, ANY, ANY, ANY],
            out_specs=(ANY, ANY),
            scratch_shapes=[
                pltpu.VMEM((CHUNK - NB, WAVES, LATS), F32),
                pltpu.VMEM((CHUNK, 2, LEVS, WAVES), F32),
                DMA((CHUNK - NB,)), DMA((CHUNK,)), DMA((CHUNK,)), DMA((EARLY_WAVES,)),
            ],
            compiler_params=pltpu.CompilerParams(vmem_limit_bytes=LIMIT_END),
            name='finish',
        )(last, leg_last, legendre, grid_mid, spec_mid)
        return grid, spec_out

    return jax.shard_map(per_device, mesh=mesh, in_specs=(P('w', None, 'lev', None), P(None, None, None), P(None)), out_specs=(P('lev', 'w', None), P('w', None, 'lev', None)), check_vma=False)
```

```python
import functools

import jax
import jax.numpy as jnp
import numpy as np
from jax import lax
from jax.experimental import pallas as pl
from jax.experimental.pallas import tpu as pltpu
from jax.sharding import PartitionSpec as P

DEVS = 8
WAVES = 512
OWN = WAVES // DEVS
LATS = 768
LAT = LATS // DEVS
LEVS = 32
LONS = 1024
HALF = LONS // 2
KK = 8
QQ = 4
SIDE = 4
LANES = QQ * LAT
CHUNK = 8
NB = 5
CHUNKS = OWN // CHUNK
FIRST = 6
EARLY = 2
AHEAD = 3
EARLY_WAVES = OWN - CHUNK
BF = jnp.bfloat16
F32 = jnp.float32


def split(x):
    hi = x.astype(BF)
    return hi, (x - hi.astype(F32)).astype(BF)


def dot3(a_hi, a_lo, b_hi, b_lo, dims):
    mm = functools.partial(lax.dot_general, dimension_numbers=(dims, ((), ())), preferred_element_type=F32)
    return mm(a_hi, b_hi) + (mm(a_hi, b_lo) + mm(a_lo, b_hi))


def dot_stacked(a, b, dims):
    rows = a.shape[0]
    (a_hi, a_lo), (b_hi, b_lo) = split(a), split(b)
    mm = functools.partial(lax.dot_general, dimension_numbers=(dims, ((), ())), preferred_element_type=F32)
    both = mm(jnp.concatenate([a_hi, a_lo], axis=0), b_hi)
    return both[:rows] + (both[rows:] + mm(a_hi, b_lo))


def barrier_signal(me):
    sem = pltpu.get_barrier_semaphore()
    for o in range(1, DEVS):
        pl.semaphore_signal(sem, inc=1, device_id={'w': lax.rem(me + o, DEVS)}, device_id_type=pl.DeviceIdType.MESH)


def barrier_wait():
    pl.semaphore_wait(pltpu.get_barrier_semaphore(), DEVS - 1)


def own_wave(t):
    return 2 * lax.rem(t, OWN // 2) + lax.div(t, OWN // 2)


def gather_rows(hbuf, i):
    rows = []
    for r in range(2):
        parts = [jnp.concatenate([hbuf[d, kk, r, pl.ds(i, 1), :] for kk in range(KK)], axis=0) for d in range(DEVS)]
        for q in range(QQ):
            rows.append(jnp.concatenate([p[:, q * LAT:(q + 1) * LAT] for p in parts], axis=1))
    return jnp.concatenate(rows, axis=0)


def whole(lbuf, slot):
    return jnp.concatenate([lbuf[slot, 0], lbuf[slot, 1]], axis=1)


def transform(coef, leg, table, weight_in, frecv, spec_out, last_out, lbuf, grid_out, dft, dft_t, weight, cbuf, fbuf, both, hrecv, csem, hsem, lsem, fsem, fs1, fr1, fs2, fr2, ssem, asem, bsem, tsem):
    me = lax.axis_index('w')
    barrier_signal(me)

    row, col = lax.div(me, SIDE), lax.rem(me, SIDE)

    def fetch_half(u):
        t = lax.div(u, 2 * CHUNK) * CHUNK + lax.rem(u, CHUNK)
        side = lax.rem(row + 1 + lax.rem(lax.div(u, CHUNK), 2), 2)
        cols = pl.ds(pl.multiple_of(side * LANES, LANES), LANES)
        buf = lax.rem(u, 2 * NB)
        return pltpu.make_async_copy(leg.at[me * OWN + own_wave(t), :, cols], lbuf.at[lax.div(buf, 2), lax.rem(buf, 2)], hsem.at[buf])

    def fetch_coef(u):
        t = lax.div(u, 2 * CHUNK) * CHUNK + lax.rem(u, CHUNK)
        slot = lax.rem(u, NB)
        return pltpu.make_async_copy(coef.at[own_wave(t)], cbuf.at[slot], csem.at[slot])

    def fetch_leg(t, half):
        slot = lax.rem(t, NB)
        cols = pl.ds(half * LANES, LANES)
        return pltpu.make_async_copy(leg.at[me * OWN + own_wave(t), :, cols], lbuf.at[slot, half], lsem.at[slot, half])

    def row_of(o):
        return row if o < SIDE else 1 - row

    def target(o):
        return row_of(o) * SIDE + lax.rem(col + o, SIDE)

    def source(o):
        return row_of(o) * SIDE + lax.rem(col - o + DEVS, SIDE)

    def block(d, row=0, size=OWN):
        return pl.ds(pl.multiple_of(d * OWN + row, CHUNK), size)

    def move(o, src_ref, dst_ref, send_sem, recv_sem):
        if o == 0:
            pltpu.make_async_copy(src_ref, dst_ref, recv_sem).start()
        else:
            pltpu.make_async_remote_copy(src_ref=src_ref, dst_ref=dst_ref, send_sem=send_sem, recv_sem=recv_sem, device_id={'w': target(o)}, device_id_type=pl.DeviceIdType.MESH).start()

    def wait_for(part, sem):
        pltpu.make_async_copy(part, part, sem).wait()

    for u in range(2 * NB):
        fetch_half(u).start()
    for u in range(NB):
        fetch_coef(u).start()
    constants = (pltpu.make_async_copy(table, dft, tsem.at[0]), pltpu.make_async_copy(weight_in, weight, tsem.at[1]))
    for copy in constants:
        copy.start()

    @pl.loop(0, CHUNKS)
    def _(c):
        for part in range(2):
            side = lax.rem(row + 1 + part, 2)

            @pl.loop(0, CHUNK)
            def _(i):
                u = (2 * c + part) * CHUNK + i
                t = c * CHUNK + i
                fetch_half(u).wait()
                fetch_coef(u).wait()
                buf = lax.rem(u, 2 * NB)
                f = dot_stacked(cbuf[lax.rem(u, NB)].reshape(2 * LEVS, WAVES), lbuf[lax.div(buf, 2), lax.rem(buf, 2)], ((1,), (0,)))

                @pl.when(u + 2 * NB < 2 * OWN)
                def _():
                    fetch_half(u + 2 * NB).start()

                @pl.when(u + NB < 2 * OWN)
                def _():
                    fetch_coef(u + NB).start()

                for j in range(SIDE):
                    cols = f[:, j * LAT:(j + 1) * LAT]
                    for r in range(2):
                        packed = jnp.concatenate([cols[r * LEVS + q * KK:r * LEVS + (q + 1) * KK] for q in range(QQ)], axis=1)
                        for kk in range(KK):
                            both[kk, r, pl.ds((side * SIDE + j) * OWN + t, 1), :] = packed[kk:kk + 1]

            if part == 0:
                @pl.when(c == 0)
                def _():
                    barrier_wait()

            for o in range(SIDE):
                o += SIDE * (1 - part)
                move(o, both.at[pl.ds(0, FIRST), :, block(target(o), c * CHUNK, CHUNK), :], frecv.at[pl.ds(0, FIRST), :, block(me, c * CHUNK, CHUNK), :], fs1.at[o], fr1.at[o])

    for kk in range(FIRST, KK):
        for o in range(DEVS):
            move(o, both.at[kk, :, block(target(o)), :], frecv.at[kk, :, block(me), :], fs2.at[kk, o], fr2.at[kk, o])
    for t in range(NB):
        for half in range(2):
            fetch_leg(t, half).start()

    for copy in constants:
        copy.wait()
    weights = weight[...].reshape(1, LATS)
    own_weight = weights[:, 0:LAT]
    for d in range(1, DEVS):
        own_weight = jnp.where(me == d, weights[:, d * LAT:(d + 1) * LAT], own_weight)
    own_weight = jnp.concatenate([own_weight] * QQ, axis=1)
    rows = lax.broadcasted_iota(jnp.int32, (WAVES, 1), 0)
    for par in range(2):
        unscale = jnp.where(rows == 0, 1.0 * LONS, 1.0 * HALF) if par == 0 else 1.0 * HALF
        for half in range(2):
            dft_t[par, half] = (dft[par, half].astype(F32).T * unscale).astype(BF)

    def dst_rows(o, row, size):
        return pl.ds(pl.multiple_of(target(o) * (OWN // 2) + row, CHUNK), size)

    def send_levels(kk):
        for o in range(DEVS):
            for par in range(2):
                move(o, both.at[kk, :, dst_rows(o, par * (WAVES // 2), OWN // 2), :], hrecv.at[me, par, kk], ssem.at[o], asem.at[o])

    def chunk_at(ref, c):
        row = pl.multiple_of(lax.rem(c, 4) * CHUNK, CHUNK)
        return ref.at[lax.div(c, 4), pl.ds(EARLY, KK - EARLY), :, pl.ds(row, CHUNK), :]

    def send_chunk(c):
        row = lax.div(c, 4) * (WAVES // 2) + lax.rem(c, 4) * CHUNK
        for o in range(DEVS):
            move(o, both.at[pl.ds(EARLY, KK - EARLY), :, dst_rows(o, row, CHUNK), :], chunk_at(hrecv.at[me], c), ssem.at[o], bsem.at[c, o])

    def arrived(c):
        for o in range(DEVS):
            wait_for(chunk_at(hrecv.at[source(o)], c), bsem.at[c, o])

    @pl.loop(0, KK)
    def _(kk):
        @pl.when(kk == 0)
        def _():
            for o in range(DEVS):
                wait_for(frecv.at[pl.ds(0, FIRST), :, block(source(o)), :], fr1.at[o])
            for o in range(1, DEVS):
                wait_for(both.at[pl.ds(0, FIRST), :, block(target(o)), :], fs1.at[o])

        @pl.when(kk >= FIRST)
        def _():
            for o in range(DEVS):
                wait_for(frecv.at[kk, :, block(source(o)), :], fr2.at[kk, o])
            for o in range(1, DEVS):
                wait_for(both.at[kk, :, block(target(o)), :], fs2.at[kk, o])

        fetch = pltpu.make_async_copy(frecv.at[kk], fbuf, fsem)
        fetch.start()
        fetch.wait()

        sums = []
        for par in range(2):
            x = jnp.concatenate([fbuf[r, d * OWN + par * (OWN // 2):d * OWN + (par + 1) * (OWN // 2), :] for r in range(2) for d in range(DEVS)], axis=0)
            x_hi, x_lo = split(x)
            sums.append(dot3(dft[par, 0], dft[par, 1], x_hi, x_lo, ((1,), (0,))))
        first, second = sums[0] + sums[1], sums[0] - sums[1]
        for half, y in enumerate((first.T, second.T)):
            for q in range(QQ):
                grid_out[q * KK + kk, :, half * HALF:(half + 1) * HALF] = y[q * LAT:(q + 1) * LAT]
        first, second = first * first, second * second
        for par, y in enumerate((first + second, first - second)):
            y_hi, y_lo = split(y)
            h = dot3(dft_t[par, 0], dft_t[par, 1], y_hi, y_lo, ((1,), (0,))) * own_weight
            for r in range(2):
                both[kk, r, par * (WAVES // 2):(par + 1) * (WAVES // 2), :] = h[r * (WAVES // 2):(r + 1) * (WAVES // 2)]

        @pl.when(kk < EARLY)
        def _():
            send_levels(kk)

    for c in range(AHEAD):
        send_chunk(c)
    for o in range(DEVS):
        wait_for(hrecv.at[source(o), :, pl.ds(0, EARLY)], asem.at[o])

    @pl.loop(0, CHUNKS - 1)
    def _(c):
        arrived(c)

        @pl.when(c + AHEAD < CHUNKS)
        def _():
            send_chunk(c + AHEAD)

        par, row = lax.div(c, 4), lax.rem(c, 4) * CHUNK

        @pl.loop(0, CHUNK)
        def _(i):
            t = c * CHUNK + i
            h = gather_rows(hrecv.at[:, par], row + i)
            for half in range(2):
                fetch_leg(t, half).wait()
            spec_out[t] = dot_stacked(h, whole(lbuf, lax.rem(t, NB)), ((1,), (1,))).reshape(2, LEVS, WAVES)

            @pl.when(t + NB < OWN)
            def _():
                for half in range(2):
                    fetch_leg(t + NB, half).start()

    arrived(CHUNKS - 1)
    for t in range(EARLY_WAVES, EARLY_WAVES + NB):
        for half in range(2):
            fetch_leg(t, half).wait()
    last_out[...] = hrecv[:, 1, :, :, 3 * CHUNK:4 * CHUNK, :]
    for o in range(1, DEVS):
        wait_for(both.at[:, :, block(target(o)), :], ssem.at[o])


def finish(h_in, leg_in, leg, grid_in, spec_in, grid_out, spec_out, lbuf, obuf, lsem, osem, gsem, ssem):
    me = lax.axis_index('w')

    def fetch_leg(i):
        return pltpu.make_async_copy(leg.at[me * OWN + own_wave(EARLY_WAVES + i)], lbuf.at[i - NB], lsem.at[i - NB])

    def grid_copy(i):
        return pltpu.make_async_copy(grid_in.at[pl.ds(i * QQ, QQ)], grid_out.at[pl.ds(i * QQ, QQ)], gsem.at[i])

    def spec_copy(t):
        return pltpu.make_async_copy(spec_in.at[t], spec_out.at[own_wave(t)], ssem.at[t])

    def store(i):
        return pltpu.make_async_copy(obuf.at[i], spec_out.at[own_wave(EARLY_WAVES + i)], osem.at[i])

    for i in range(NB, CHUNK):
        fetch_leg(i).start()
    for i in range(CHUNK):
        grid_copy(i).start()

    @pl.loop(0, EARLY_WAVES)
    def _(t):
        spec_copy(t).start()

    @pl.loop(0, NB)
    def _(i):
        block = whole(leg_in, lax.rem(EARLY_WAVES + i, NB))
        obuf[i] = dot_stacked(gather_rows(h_in, i), block, ((1,), (1,))).reshape(2, LEVS, WAVES)
        store(i).start()

    @pl.loop(NB, CHUNK)
    def _(i):
        h = gather_rows(h_in, i)
        fetch_leg(i).wait()
        obuf[i] = dot_stacked(h, lbuf[i - NB], ((1,), (1,))).reshape(2, LEVS, WAVES)
        store(i).start()

    @pl.loop(0, CHUNK)
    def _(i):
        store(i).wait()
        grid_copy(i).wait()

    @pl.loop(0, EARLY_WAVES)
    def _(t):
        spec_copy(t).wait()


def dft_tables():
    n = np.arange(HALF)[:, None]
    tabs = []
    for par in range(2):
        m = np.arange(par, WAVES, 2)[None, :]
        ang = 2 * np.pi * ((m * n) % LONS) / LONS
        tabs.append(np.concatenate([np.cos(ang), -np.sin(ang)], axis=1))
    back = np.stack(tabs)
    scale = np.full((2, 1, WAVES), 2.0 / LONS)
    scale[0, 0, 0] = 1.0 / LONS
    scale[0, 0, WAVES // 2] = 0.0

    def halves(x):
        x = x.astype(np.float32)
        hi = x.astype(jnp.bfloat16)
        return np.stack([hi, (x - hi.astype(np.float32)).astype(jnp.bfloat16)], axis=1)

    return halves(back * scale)


ANY = pl.BlockSpec(memory_space=pl.ANY)
VM = pl.BlockSpec(memory_space=pltpu.VMEM)
DMA = pltpu.SemaphoreType.DMA
LIMIT = 35 * 1024 * 1024
LIMIT_END = 18 * 1024 * 1024


def solution(mesh):
    table = dft_tables()

    def per_device(coef, legendre, gauss_weight):
        _, spec_mid, last, leg_last, grid_mid = pl.pallas_call(
            transform,
            out_shape=(
                jax.ShapeDtypeStruct((KK, 2, WAVES, LANES), F32),
                pltpu.VMEM((EARLY_WAVES, 2, LEVS, WAVES), F32),
                pltpu.VMEM((DEVS, KK, 2, CHUNK, LANES), F32),
                pltpu.VMEM((NB, 2, WAVES, LANES), F32),
                pltpu.VMEM((LEVS, LAT, LONS), F32),
            ),
            in_specs=[ANY, ANY, ANY, ANY],
            out_specs=(ANY, VM, VM, VM, VM),
            scratch_shapes=[
                pltpu.VMEM((2, 2, HALF, WAVES), BF),
                pltpu.VMEM((2, 2, WAVES, HALF), BF),
                pltpu.VMEM((LATS,), F32),
                pltpu.VMEM((NB, 2, LEVS, WAVES), F32),
                pltpu.VMEM((2, WAVES, LANES), F32),
                pltpu.VMEM((KK, 2, WAVES, LANES), F32),
                pltpu.VMEM((DEVS, 2, KK, 2, OWN // 2, LANES), F32),
                DMA((NB,)), DMA((2 * NB,)), DMA((NB, 2)), DMA,
                DMA((DEVS,)), DMA((DEVS,)), DMA((KK, DEVS)), DMA((KK, DEVS)), DMA((DEVS,)), DMA((DEVS,)), DMA((CHUNKS, DEVS)), DMA((2,)),
            ],
            compiler_params=pltpu.CompilerParams(collective_id=0, has_side_effects=True, vmem_limit_bytes=LIMIT),
            name='transform',
        )(coef, legendre, table, gauss_weight)
        grid, spec_out = pl.pallas_call(
            finish,
            out_shape=(jax.ShapeDtypeStruct((LEVS, LAT, LONS), F32), jax.ShapeDtypeStruct((OWN, 2, LEVS, WAVES), F32)),
            in_specs=[VM, VM, ANY, ANY, ANY],
            out_specs=(ANY, ANY),
            scratch_shapes=[
                pltpu.VMEM((CHUNK - NB, WAVES, LATS), F32),
                pltpu.VMEM((CHUNK, 2, LEVS, WAVES), F32),
                DMA((CHUNK - NB,)), DMA((CHUNK,)), DMA((CHUNK,)), DMA((EARLY_WAVES,)),
            ],
            compiler_params=pltpu.CompilerParams(vmem_limit_bytes=LIMIT_END),
            name='finish',
        )(last, leg_last, legendre, grid_mid, spec_mid)
        return grid, spec_out

    return jax.shard_map(per_device, mesh=mesh, in_specs=(P('w', None, 'lev', None), P(None, None, None), P(None)), out_specs=(P('lev', 'w', None), P('w', None, 'lev', None)), check_vma=False)
```

```python
import functools

import jax
import jax.numpy as jnp
import numpy as np
from jax import lax
from jax.experimental import pallas as pl
from jax.experimental.pallas import tpu as pltpu
from jax.sharding import PartitionSpec as P

DEVS = 8
WAVES = 512
OWN = WAVES // DEVS
LATS = 768
LAT = LATS // DEVS
LEVS = 32
LONS = 1024
HALF = LONS // 2
KK = 8
QQ = 4
SIDE = 4
LANES = QQ * LAT
CHUNK = 8
NB = 5
CHUNKS = OWN // CHUNK
FIRST = 6
EARLY = 2
AHEAD = 6
EARLY_WAVES = OWN - CHUNK
BF = jnp.bfloat16
F32 = jnp.float32


def split(x):
    hi = x.astype(BF)
    return hi, (x - hi.astype(F32)).astype(BF)


def dot3(a_hi, a_lo, b_hi, b_lo, dims):
    mm = functools.partial(lax.dot_general, dimension_numbers=(dims, ((), ())), preferred_element_type=F32)
    return mm(a_hi, b_hi) + (mm(a_hi, b_lo) + mm(a_lo, b_hi))


def dot_stacked(a, b, dims):
    rows = a.shape[0]
    (a_hi, a_lo), (b_hi, b_lo) = split(a), split(b)
    mm = functools.partial(lax.dot_general, dimension_numbers=(dims, ((), ())), preferred_element_type=F32)
    both = mm(jnp.concatenate([a_hi, a_lo], axis=0), b_hi)
    return both[:rows] + (both[rows:] + mm(a_hi, b_lo))


def barrier_signal(me):
    sem = pltpu.get_barrier_semaphore()
    for o in range(1, DEVS):
        pl.semaphore_signal(sem, inc=1, device_id={'w': lax.rem(me + o, DEVS)}, device_id_type=pl.DeviceIdType.MESH)


def barrier_wait():
    pl.semaphore_wait(pltpu.get_barrier_semaphore(), DEVS - 1)


def own_wave(t):
    return 2 * lax.rem(t, OWN // 2) + lax.div(t, OWN // 2)


def gather_rows(hbuf, i):
    rows = []
    for r in range(2):
        parts = [jnp.concatenate([hbuf[d, kk, r, pl.ds(i, 1), :] for kk in range(KK)], axis=0) for d in range(DEVS)]
        for q in range(QQ):
            rows.append(jnp.concatenate([p[:, q * LAT:(q + 1) * LAT] for p in parts], axis=1))
    return jnp.concatenate(rows, axis=0)


def whole(lbuf, slot):
    return jnp.concatenate([lbuf[slot, 0], lbuf[slot, 1]], axis=1)


def transform(coef, leg, table, weight_in, frecv, spec_out, last_out, lbuf, grid_out, dft, dft_t, weight, cbuf, fbuf, both, hrecv, csem, hsem, lsem, fsem, fs1, fr1, fs2, fr2, ssem, asem, bsem, tsem):
    me = lax.axis_index('w')
    barrier_signal(me)

    row, col = lax.div(me, SIDE), lax.rem(me, SIDE)

    def fetch_half(u):
        t = lax.div(u, 2 * CHUNK) * CHUNK + lax.rem(u, CHUNK)
        side = lax.rem(row + 1 + lax.rem(lax.div(u, CHUNK), 2), 2)
        cols = pl.ds(pl.multiple_of(side * LANES, LANES), LANES)
        buf = lax.rem(u, 2 * NB)
        return pltpu.make_async_copy(leg.at[me * OWN + own_wave(t), :, cols], lbuf.at[lax.div(buf, 2), lax.rem(buf, 2)], hsem.at[buf])

    def fetch_coef(u):
        t = lax.div(u, 2 * CHUNK) * CHUNK + lax.rem(u, CHUNK)
        slot = lax.rem(u, NB)
        return pltpu.make_async_copy(coef.at[own_wave(t)], cbuf.at[slot], csem.at[slot])

    def fetch_leg(t, half):
        slot = lax.rem(t, NB)
        cols = pl.ds(half * LANES, LANES)
        return pltpu.make_async_copy(leg.at[me * OWN + own_wave(t), :, cols], lbuf.at[slot, half], lsem.at[slot, half])

    def row_of(o):
        return row if o < SIDE else 1 - row

    def target(o):
        return row_of(o) * SIDE + lax.rem(col + o, SIDE)

    def source(o):
        return row_of(o) * SIDE + lax.rem(col - o + DEVS, SIDE)

    def block(d, row=0, size=OWN):
        return pl.ds(pl.multiple_of(d * OWN + row, CHUNK), size)

    def move(o, src_ref, dst_ref, send_sem, recv_sem):
        if o == 0:
            pltpu.make_async_copy(src_ref, dst_ref, recv_sem).start()
        else:
            pltpu.make_async_remote_copy(src_ref=src_ref, dst_ref=dst_ref, send_sem=send_sem, recv_sem=recv_sem, device_id={'w': target(o)}, device_id_type=pl.DeviceIdType.MESH).start()

    def wait_for(part, sem):
        pltpu.make_async_copy(part, part, sem).wait()

    for u in range(NB):
        fetch_coef(u).start()
    for u in range(2 * NB):
        fetch_half(u).start()
    constants = (pltpu.make_async_copy(table, dft, tsem.at[0]), pltpu.make_async_copy(weight_in, weight, tsem.at[1]))
    for copy in constants:
        copy.start()

    @pl.loop(0, CHUNKS)
    def _(c):
        for part in range(2):
            side = lax.rem(row + 1 + part, 2)

            @pl.loop(0, CHUNK)
            def _(i):
                u = (2 * c + part) * CHUNK + i
                t = c * CHUNK + i
                fetch_half(u).wait()
                fetch_coef(u).wait()
                buf = lax.rem(u, 2 * NB)
                f = dot_stacked(cbuf[lax.rem(u, NB)].reshape(2 * LEVS, WAVES), lbuf[lax.div(buf, 2), lax.rem(buf, 2)], ((1,), (0,)))

                @pl.when(u + 2 * NB < 2 * OWN)
                def _():
                    fetch_half(u + 2 * NB).start()

                @pl.when(u + NB < 2 * OWN)
                def _():
                    fetch_coef(u + NB).start()

                for j in range(SIDE):
                    cols = f[:, j * LAT:(j + 1) * LAT]
                    for r in range(2):
                        packed = jnp.concatenate([cols[r * LEVS + q * KK:r * LEVS + (q + 1) * KK] for q in range(QQ)], axis=1)
                        for kk in range(KK):
                            both[kk, r, pl.ds((side * SIDE + j) * OWN + t, 1), :] = packed[kk:kk + 1]

            if part == 0:
                @pl.when(c == 0)
                def _():
                    barrier_wait()

            for o in range(SIDE):
                o += SIDE * (1 - part)
                move(o, both.at[pl.ds(0, FIRST), :, block(target(o), c * CHUNK, CHUNK), :], frecv.at[pl.ds(0, FIRST), :, block(me, c * CHUNK, CHUNK), :], fs1.at[o], fr1.at[o])

    for kk in range(FIRST, KK):
        for o in range(DEVS):
            move(o, both.at[kk, :, block(target(o)), :], frecv.at[kk, :, block(me), :], fs2.at[kk, o], fr2.at[kk, o])
    for t in range(NB):
        for half in range(2):
            fetch_leg(t, half).start()

    for copy in constants:
        copy.wait()
    weights = weight[...].reshape(1, LATS)
    own_weight = weights[:, 0:LAT]
    for d in range(1, DEVS):
        own_weight = jnp.where(me == d, weights[:, d * LAT:(d + 1) * LAT], own_weight)
    own_weight = jnp.concatenate([own_weight] * QQ, axis=1)
    rows = lax.broadcasted_iota(jnp.int32, (WAVES, 1), 0)
    for par in range(2):
        unscale = jnp.where(rows == 0, 1.0 * LONS, 1.0 * HALF) if par == 0 else 1.0 * HALF
        for half in range(2):
            dft_t[par, half] = (dft[par, half].astype(F32).T * unscale).astype(BF)

    def dst_rows(o, row, size):
        return pl.ds(pl.multiple_of(target(o) * (OWN // 2) + row, CHUNK), size)

    def send_levels(kk):
        for o in range(DEVS):
            for par in range(2):
                move(o, both.at[kk, :, dst_rows(o, par * (WAVES // 2), OWN // 2), :], hrecv.at[me, par, kk], ssem.at[o], asem.at[o])

    def chunk_at(ref, c):
        row = pl.multiple_of(lax.rem(c, 4) * CHUNK, CHUNK)
        return ref.at[lax.div(c, 4), pl.ds(EARLY, KK - EARLY), :, pl.ds(row, CHUNK), :]

    def send_chunk(c):
        row = lax.div(c, 4) * (WAVES // 2) + lax.rem(c, 4) * CHUNK
        for o in range(DEVS):
            move(o, both.at[pl.ds(EARLY, KK - EARLY), :, dst_rows(o, row, CHUNK), :], chunk_at(hrecv.at[me], c), ssem.at[o], bsem.at[c, o])

    def arrived(c):
        for o in range(DEVS):
            wait_for(chunk_at(hrecv.at[source(o)], c), bsem.at[c, o])

    @pl.loop(0, KK)
    def _(kk):
        @pl.when(kk == 0)
        def _():
            for o in range(DEVS):
                wait_for(frecv.at[pl.ds(0, FIRST), :, block(source(o)), :], fr1.at[o])
            for o in range(1, DEVS):
                wait_for(both.at[pl.ds(0, FIRST), :, block(target(o)), :], fs1.at[o])

        @pl.when(kk >= FIRST)
        def _():
            for o in range(DEVS):
                wait_for(frecv.at[kk, :, block(source(o)), :], fr2.at[kk, o])
            for o in range(1, DEVS):
                wait_for(both.at[kk, :, block(target(o)), :], fs2.at[kk, o])

        fetch = pltpu.make_async_copy(frecv.at[kk], fbuf, fsem)
        fetch.start()
        fetch.wait()

        sums = []
        for par in range(2):
            x = jnp.concatenate([fbuf[r, d * OWN + par * (OWN // 2):d * OWN + (par + 1) * (OWN // 2), :] for r in range(2) for d in range(DEVS)], axis=0)
            x_hi, x_lo = split(x)
            sums.append(dot3(dft[par, 0], dft[par, 1], x_hi, x_lo, ((1,), (0,))))
        first, second = sums[0] + sums[1], sums[0] - sums[1]
        for half, y in enumerate((first.T, second.T)):
            for q in range(QQ):
                grid_out[q * KK + kk, :, half * HALF:(half + 1) * HALF] = y[q * LAT:(q + 1) * LAT]
        first, second = first * first, second * second
        for par, y in enumerate((first + second, first - second)):
            y_hi, y_lo = split(y)
            h = dot3(dft_t[par, 0], dft_t[par, 1], y_hi, y_lo, ((1,), (0,))) * own_weight
            for r in range(2):
                both[kk, r, par * (WAVES // 2):(par + 1) * (WAVES // 2), :] = h[r * (WAVES // 2):(r + 1) * (WAVES // 2)]

        @pl.when(kk < EARLY)
        def _():
            send_levels(kk)

    for c in range(AHEAD):
        send_chunk(c)
    for o in range(DEVS):
        wait_for(hrecv.at[source(o), :, pl.ds(0, EARLY)], asem.at[o])

    @pl.loop(0, CHUNKS - 1)
    def _(c):
        arrived(c)

        @pl.when(c + AHEAD < CHUNKS)
        def _():
            send_chunk(c + AHEAD)

        par, row = lax.div(c, 4), lax.rem(c, 4) * CHUNK

        @pl.loop(0, CHUNK)
        def _(i):
            t = c * CHUNK + i
            h = gather_rows(hrecv.at[:, par], row + i)
            for half in range(2):
                fetch_leg(t, half).wait()
            spec_out[t] = dot_stacked(h, whole(lbuf, lax.rem(t, NB)), ((1,), (1,))).reshape(2, LEVS, WAVES)

            @pl.when(t + NB < OWN)
            def _():
                for half in range(2):
                    fetch_leg(t + NB, half).start()

    arrived(CHUNKS - 1)
    for t in range(EARLY_WAVES, EARLY_WAVES + NB):
        for half in range(2):
            fetch_leg(t, half).wait()
    last_out[...] = hrecv[:, 1, :, :, 3 * CHUNK:4 * CHUNK, :]
    for o in range(1, DEVS):
        wait_for(both.at[:, :, block(target(o)), :], ssem.at[o])


def finish(h_in, leg_in, leg, grid_in, spec_in, grid_out, spec_out, lbuf, obuf, lsem, osem, gsem, ssem):
    me = lax.axis_index('w')

    def fetch_leg(i):
        return pltpu.make_async_copy(leg.at[me * OWN + own_wave(EARLY_WAVES + i)], lbuf.at[i - NB], lsem.at[i - NB])

    def grid_copy(i):
        return pltpu.make_async_copy(grid_in.at[pl.ds(i * QQ, QQ)], grid_out.at[pl.ds(i * QQ, QQ)], gsem.at[i])

    def spec_copy(t):
        return pltpu.make_async_copy(spec_in.at[t], spec_out.at[own_wave(t)], ssem.at[t])

    def store(i):
        return pltpu.make_async_copy(obuf.at[i], spec_out.at[own_wave(EARLY_WAVES + i)], osem.at[i])

    for i in range(NB, CHUNK):
        fetch_leg(i).start()
    for i in range(CHUNK):
        grid_copy(i).start()

    @pl.loop(0, EARLY_WAVES)
    def _(t):
        spec_copy(t).start()

    @pl.loop(0, NB)
    def _(i):
        block = whole(leg_in, lax.rem(EARLY_WAVES + i, NB))
        obuf[i] = dot_stacked(gather_rows(h_in, i), block, ((1,), (1,))).reshape(2, LEVS, WAVES)
        store(i).start()

    @pl.loop(NB, CHUNK)
    def _(i):
        h = gather_rows(h_in, i)
        fetch_leg(i).wait()
        obuf[i] = dot_stacked(h, lbuf[i - NB], ((1,), (1,))).reshape(2, LEVS, WAVES)
        store(i).start()

    @pl.loop(0, CHUNK)
    def _(i):
        store(i).wait()
        grid_copy(i).wait()

    @pl.loop(0, EARLY_WAVES)
    def _(t):
        spec_copy(t).wait()


def dft_tables():
    n = np.arange(HALF)[:, None]
    tabs = []
    for par in range(2):
        m = np.arange(par, WAVES, 2)[None, :]
        ang = 2 * np.pi * ((m * n) % LONS) / LONS
        tabs.append(np.concatenate([np.cos(ang), -np.sin(ang)], axis=1))
    back = np.stack(tabs)
    scale = np.full((2, 1, WAVES), 2.0 / LONS)
    scale[0, 0, 0] = 1.0 / LONS
    scale[0, 0, WAVES // 2] = 0.0

    def halves(x):
        x = x.astype(np.float32)
        hi = x.astype(jnp.bfloat16)
        return np.stack([hi, (x - hi.astype(np.float32)).astype(jnp.bfloat16)], axis=1)

    return halves(back * scale)


ANY = pl.BlockSpec(memory_space=pl.ANY)
VM = pl.BlockSpec(memory_space=pltpu.VMEM)
DMA = pltpu.SemaphoreType.DMA
LIMIT = 35 * 1024 * 1024
LIMIT_END = 18 * 1024 * 1024


def solution(mesh):
    table = dft_tables()

    def per_device(coef, legendre, gauss_weight):
        _, spec_mid, last, leg_last, grid_mid = pl.pallas_call(
            transform,
            out_shape=(
                jax.ShapeDtypeStruct((KK, 2, WAVES, LANES), F32),
                pltpu.VMEM((EARLY_WAVES, 2, LEVS, WAVES), F32),
                pltpu.VMEM((DEVS, KK, 2, CHUNK, LANES), F32),
                pltpu.VMEM((NB, 2, WAVES, LANES), F32),
                pltpu.VMEM((LEVS, LAT, LONS), F32),
            ),
            in_specs=[ANY, ANY, ANY, ANY],
            out_specs=(ANY, VM, VM, VM, VM),
            scratch_shapes=[
                pltpu.VMEM((2, 2, HALF, WAVES), BF),
                pltpu.VMEM((2, 2, WAVES, HALF), BF),
                pltpu.VMEM((LATS,), F32),
                pltpu.VMEM((NB, 2, LEVS, WAVES), F32),
                pltpu.VMEM((2, WAVES, LANES), F32),
                pltpu.VMEM((KK, 2, WAVES, LANES), F32),
                pltpu.VMEM((DEVS, 2, KK, 2, OWN // 2, LANES), F32),
                DMA((NB,)), DMA((2 * NB,)), DMA((NB, 2)), DMA,
                DMA((DEVS,)), DMA((DEVS,)), DMA((KK, DEVS)), DMA((KK, DEVS)), DMA((DEVS,)), DMA((DEVS,)), DMA((CHUNKS, DEVS)), DMA((2,)),
            ],
            compiler_params=pltpu.CompilerParams(collective_id=0, has_side_effects=True, vmem_limit_bytes=LIMIT),
            name='transform',
        )(coef, legendre, table, gauss_weight)
        grid, spec_out = pl.pallas_call(
            finish,
            out_shape=(jax.ShapeDtypeStruct((LEVS, LAT, LONS), F32), jax.ShapeDtypeStruct((OWN, 2, LEVS, WAVES), F32)),
            in_specs=[VM, VM, ANY, ANY, ANY],
            out_specs=(ANY, ANY),
            scratch_shapes=[
                pltpu.VMEM((CHUNK - NB, WAVES, LATS), F32),
                pltpu.VMEM((CHUNK, 2, LEVS, WAVES), F32),
                DMA((CHUNK - NB,)), DMA((CHUNK,)), DMA((CHUNK,)), DMA((EARLY_WAVES,)),
            ],
            compiler_params=pltpu.CompilerParams(vmem_limit_bytes=LIMIT_END),
            name='finish',
        )(last, leg_last, legendre, grid_mid, spec_mid)
        return grid, spec_out

    return jax.shard_map(per_device, mesh=mesh, in_specs=(P('w', None, 'lev', None), P(None, None, None), P(None)), out_specs=(P('lev', 'w', None), P('w', None, 'lev', None)), check_vma=False)
```

```python
import functools

import jax
import jax.numpy as jnp
import numpy as np
from jax import lax
from jax.experimental import pallas as pl
from jax.experimental.pallas import tpu as pltpu
from jax.sharding import PartitionSpec as P

DEVS = 8
WAVES = 512
OWN = WAVES // DEVS
LATS = 768
LAT = LATS // DEVS
LEVS = 32
LONS = 1024
HALF = LONS // 2
KK = 8
QQ = 4
ORDER = (6, 5, 7, 4, 2, 3, 1, 0)
SIDE = 4
LANES = QQ * LAT
CHUNK = 8
NB = 5
CHUNKS = OWN // CHUNK
FIRST = 6
EARLY = 2
AHEAD = 6
EARLY_WAVES = OWN - CHUNK
BF = jnp.bfloat16
F32 = jnp.float32


def split(x):
    hi = x.astype(BF)
    return hi, (x - hi.astype(F32)).astype(BF)


def dot3(a_hi, a_lo, b_hi, b_lo, dims):
    mm = functools.partial(lax.dot_general, dimension_numbers=(dims, ((), ())), preferred_element_type=F32)
    return mm(a_hi, b_hi) + (mm(a_hi, b_lo) + mm(a_lo, b_hi))


def dot_stacked(a, b, dims):
    rows = a.shape[0]
    (a_hi, a_lo), (b_hi, b_lo) = split(a), split(b)
    mm = functools.partial(lax.dot_general, dimension_numbers=(dims, ((), ())), preferred_element_type=F32)
    both = mm(jnp.concatenate([a_hi, a_lo], axis=0), b_hi)
    return both[:rows] + (both[rows:] + mm(a_hi, b_lo))


def barrier_signal(me):
    sem = pltpu.get_barrier_semaphore()
    for o in range(1, DEVS):
        pl.semaphore_signal(sem, inc=1, device_id={'w': lax.rem(me + o, DEVS)}, device_id_type=pl.DeviceIdType.MESH)


def barrier_wait():
    pl.semaphore_wait(pltpu.get_barrier_semaphore(), DEVS - 1)


def own_wave(t):
    return 2 * lax.rem(t, OWN // 2) + lax.div(t, OWN // 2)


def gather_rows(hbuf, i):
    rows = []
    for r in range(2):
        parts = [jnp.concatenate([hbuf[d, kk, r, pl.ds(i, 1), :] for kk in range(KK)], axis=0) for d in range(DEVS)]
        for q in range(QQ):
            rows.append(jnp.concatenate([p[:, q * LAT:(q + 1) * LAT] for p in parts], axis=1))
    return jnp.concatenate(rows, axis=0)


def whole(lbuf, slot):
    return jnp.concatenate([lbuf[slot, 0], lbuf[slot, 1]], axis=1)


def transform(coef, leg, table, weight_in, frecv, spec_out, last_out, lbuf, grid_out, dft, dft_t, weight, cbuf, fbuf, both, hrecv, csem, hsem, lsem, fsem, fs1, fr1, fs2, fr2, ssem, asem, bsem, tsem):
    me = lax.axis_index('w')
    barrier_signal(me)

    row, col = lax.div(me, SIDE), lax.rem(me, SIDE)

    def fetch_half(u):
        t = lax.div(u, 2 * CHUNK) * CHUNK + lax.rem(u, CHUNK)
        side = lax.rem(row + 1 + lax.rem(lax.div(u, CHUNK), 2), 2)
        cols = pl.ds(pl.multiple_of(side * LANES, LANES), LANES)
        buf = lax.rem(u, 2 * NB)
        return pltpu.make_async_copy(leg.at[me * OWN + own_wave(t), :, cols], lbuf.at[lax.div(buf, 2), lax.rem(buf, 2)], hsem.at[buf])

    def fetch_coef(u):
        t = lax.div(u, 2 * CHUNK) * CHUNK + lax.rem(u, CHUNK)
        slot = lax.rem(u, NB)
        return pltpu.make_async_copy(coef.at[own_wave(t)], cbuf.at[slot], csem.at[slot])

    def fetch_leg(t, half):
        slot = lax.rem(t, NB)
        cols = pl.ds(half * LANES, LANES)
        return pltpu.make_async_copy(leg.at[me * OWN + own_wave(t), :, cols], lbuf.at[slot, half], lsem.at[slot, half])

    def row_of(o):
        return row if o < SIDE else 1 - row

    def target(o):
        return row_of(o) * SIDE + lax.rem(col + o, SIDE)

    def source(o):
        return row_of(o) * SIDE + lax.rem(col - o + DEVS, SIDE)

    def block(d, row=0, size=OWN):
        return pl.ds(pl.multiple_of(d * OWN + row, CHUNK), size)

    def move(o, src_ref, dst_ref, send_sem, recv_sem):
        if o == 0:
            pltpu.make_async_copy(src_ref, dst_ref, recv_sem).start()
        else:
            pltpu.make_async_remote_copy(src_ref=src_ref, dst_ref=dst_ref, send_sem=send_sem, recv_sem=recv_sem, device_id={'w': target(o)}, device_id_type=pl.DeviceIdType.MESH).start()

    def wait_for(part, sem):
        pltpu.make_async_copy(part, part, sem).wait()

    for u in range(NB):
        fetch_coef(u).start()
    for u in range(2 * NB):
        fetch_half(u).start()
    constants = (pltpu.make_async_copy(table, dft, tsem.at[0]), pltpu.make_async_copy(weight_in, weight, tsem.at[1]))
    for copy in constants:
        copy.start()

    @pl.loop(0, CHUNKS)
    def _(c):
        for part in range(2):
            side = lax.rem(row + 1 + part, 2)

            @pl.loop(0, CHUNK)
            def _(i):
                u = (2 * c + part) * CHUNK + i
                t = c * CHUNK + i
                fetch_half(u).wait()
                fetch_coef(u).wait()
                buf = lax.rem(u, 2 * NB)
                f = dot_stacked(cbuf[lax.rem(u, NB)].reshape(2 * LEVS, WAVES), lbuf[lax.div(buf, 2), lax.rem(buf, 2)], ((1,), (0,)))

                @pl.when(u + 2 * NB < 2 * OWN)
                def _():
                    fetch_half(u + 2 * NB).start()

                @pl.when(u + NB < 2 * OWN)
                def _():
                    fetch_coef(u + NB).start()

                for j in range(SIDE):
                    cols = f[:, j * LAT:(j + 1) * LAT]
                    for r in range(2):
                        packed = jnp.concatenate([cols[r * LEVS + q * KK:r * LEVS + (q + 1) * KK] for q in range(QQ)], axis=1)
                        for kk in range(KK):
                            both[kk, r, pl.ds((side * SIDE + j) * OWN + t, 1), :] = packed[kk:kk + 1]

            if part == 0:
                @pl.when(c == 0)
                def _():
                    barrier_wait()

            for o in ORDER[part * SIDE:(part + 1) * SIDE]:
                move(o, both.at[pl.ds(0, FIRST), :, block(target(o), c * CHUNK, CHUNK), :], frecv.at[pl.ds(0, FIRST), :, block(me, c * CHUNK, CHUNK), :], fs1.at[o], fr1.at[o])

    for kk in range(FIRST, KK):
        for o in ORDER:
            move(o, both.at[kk, :, block(target(o)), :], frecv.at[kk, :, block(me), :], fs2.at[kk, o], fr2.at[kk, o])
    for t in range(NB):
        for half in range(2):
            fetch_leg(t, half).start()

    for copy in constants:
        copy.wait()
    weights = weight[...].reshape(1, LATS)
    own_weight = weights[:, 0:LAT]
    for d in range(1, DEVS):
        own_weight = jnp.where(me == d, weights[:, d * LAT:(d + 1) * LAT], own_weight)
    own_weight = jnp.concatenate([own_weight] * QQ, axis=1)
    rows = lax.broadcasted_iota(jnp.int32, (WAVES, 1), 0)
    for par in range(2):
        unscale = jnp.where(rows == 0, 1.0 * LONS, 1.0 * HALF) if par == 0 else 1.0 * HALF
        for half in range(2):
            dft_t[par, half] = (dft[par, half].astype(F32).T * unscale).astype(BF)

    def dst_rows(o, row, size):
        return pl.ds(pl.multiple_of(target(o) * (OWN // 2) + row, CHUNK), size)

    def send_levels(kk):
        for o in ORDER:
            for par in range(2):
                move(o, both.at[kk, :, dst_rows(o, par * (WAVES // 2), OWN // 2), :], hrecv.at[me, par, kk], ssem.at[o], asem.at[o])

    def chunk_at(ref, c):
        row = pl.multiple_of(lax.rem(c, 4) * CHUNK, CHUNK)
        return ref.at[lax.div(c, 4), pl.ds(EARLY, KK - EARLY), :, pl.ds(row, CHUNK), :]

    def send_chunk(c):
        row = lax.div(c, 4) * (WAVES // 2) + lax.rem(c, 4) * CHUNK
        for o in ORDER:
            move(o, both.at[pl.ds(EARLY, KK - EARLY), :, dst_rows(o, row, CHUNK), :], chunk_at(hrecv.at[me], c), ssem.at[o], bsem.at[c, o])

    def arrived(c):
        for o in range(DEVS):
            wait_for(chunk_at(hrecv.at[source(o)], c), bsem.at[c, o])

    @pl.loop(0, KK)
    def _(kk):
        @pl.when(kk == 0)
        def _():
            for o in range(DEVS):
                wait_for(frecv.at[pl.ds(0, FIRST), :, block(source(o)), :], fr1.at[o])
            for o in range(1, DEVS):
                wait_for(both.at[pl.ds(0, FIRST), :, block(target(o)), :], fs1.at[o])

        @pl.when(kk >= FIRST)
        def _():
            for o in range(DEVS):
                wait_for(frecv.at[kk, :, block(source(o)), :], fr2.at[kk, o])
            for o in range(1, DEVS):
                wait_for(both.at[kk, :, block(target(o)), :], fs2.at[kk, o])

        fetch = pltpu.make_async_copy(frecv.at[kk], fbuf, fsem)
        fetch.start()
        fetch.wait()

        sums = []
        for par in range(2):
            x = jnp.concatenate([fbuf[r, d * OWN + par * (OWN // 2):d * OWN + (par + 1) * (OWN // 2), :] for r in range(2) for d in range(DEVS)], axis=0)
            x_hi, x_lo = split(x)
            sums.append(dot3(dft[par, 0], dft[par, 1], x_hi, x_lo, ((1,), (0,))))
        first, second = sums[0] + sums[1], sums[0] - sums[1]
        for half, y in enumerate((first.T, second.T)):
            for q in range(QQ):
                grid_out[q * KK + kk, :, half * HALF:(half + 1) * HALF] = y[q * LAT:(q + 1) * LAT]
        first, second = first * first, second * second
        for par, y in enumerate((first + second, first - second)):
            y_hi, y_lo = split(y)
            h = dot3(dft_t[par, 0], dft_t[par, 1], y_hi, y_lo, ((1,), (0,))) * own_weight
            for r in range(2):
                both[kk, r, par * (WAVES // 2):(par + 1) * (WAVES // 2), :] = h[r * (WAVES // 2):(r + 1) * (WAVES // 2)]

        @pl.when(kk < EARLY)
        def _():
            send_levels(kk)

    for c in range(AHEAD):
        send_chunk(c)
    for o in range(DEVS):
        wait_for(hrecv.at[source(o), :, pl.ds(0, EARLY)], asem.at[o])

    @pl.loop(0, CHUNKS - 1)
    def _(c):
        arrived(c)

        @pl.when(c + AHEAD < CHUNKS)
        def _():
            send_chunk(c + AHEAD)

        par, row = lax.div(c, 4), lax.rem(c, 4) * CHUNK

        @pl.loop(0, CHUNK)
        def _(i):
            t = c * CHUNK + i
            h = gather_rows(hrecv.at[:, par], row + i)
            for half in range(2):
                fetch_leg(t, half).wait()
            spec_out[t] = dot_stacked(h, whole(lbuf, lax.rem(t, NB)), ((1,), (1,))).reshape(2, LEVS, WAVES)

            @pl.when(t + NB < OWN)
            def _():
                for half in range(2):
                    fetch_leg(t + NB, half).start()

    arrived(CHUNKS - 1)
    for t in range(EARLY_WAVES, EARLY_WAVES + NB):
        for half in range(2):
            fetch_leg(t, half).wait()
    last_out[...] = hrecv[:, 1, :, :, 3 * CHUNK:4 * CHUNK, :]
    for o in range(1, DEVS):
        wait_for(both.at[:, :, block(target(o)), :], ssem.at[o])


def finish(h_in, leg_in, leg, grid_in, spec_in, grid_out, spec_out, lbuf, obuf, lsem, osem, gsem, ssem):
    me = lax.axis_index('w')

    def fetch_leg(i):
        return pltpu.make_async_copy(leg.at[me * OWN + own_wave(EARLY_WAVES + i)], lbuf.at[i - NB], lsem.at[i - NB])

    def grid_copy(i):
        return pltpu.make_async_copy(grid_in.at[pl.ds(i * QQ, QQ)], grid_out.at[pl.ds(i * QQ, QQ)], gsem.at[i])

    def spec_copy(t):
        return pltpu.make_async_copy(spec_in.at[t], spec_out.at[own_wave(t)], ssem.at[t])

    def store(i):
        return pltpu.make_async_copy(obuf.at[i], spec_out.at[own_wave(EARLY_WAVES + i)], osem.at[i])

    for i in range(NB, CHUNK):
        fetch_leg(i).start()
    for i in range(CHUNK):
        grid_copy(i).start()

    @pl.loop(0, EARLY_WAVES)
    def _(t):
        spec_copy(t).start()

    @pl.loop(0, NB)
    def _(i):
        block = whole(leg_in, lax.rem(EARLY_WAVES + i, NB))
        obuf[i] = dot_stacked(gather_rows(h_in, i), block, ((1,), (1,))).reshape(2, LEVS, WAVES)
        store(i).start()

    @pl.loop(NB, CHUNK)
    def _(i):
        h = gather_rows(h_in, i)
        fetch_leg(i).wait()
        obuf[i] = dot_stacked(h, lbuf[i - NB], ((1,), (1,))).reshape(2, LEVS, WAVES)
        store(i).start()

    @pl.loop(0, CHUNK)
    def _(i):
        store(i).wait()
        grid_copy(i).wait()

    @pl.loop(0, EARLY_WAVES)
    def _(t):
        spec_copy(t).wait()


def dft_tables():
    n = np.arange(HALF)[:, None]
    tabs = []
    for par in range(2):
        m = np.arange(par, WAVES, 2)[None, :]
        ang = 2 * np.pi * ((m * n) % LONS) / LONS
        tabs.append(np.concatenate([np.cos(ang), -np.sin(ang)], axis=1))
    back = np.stack(tabs)
    scale = np.full((2, 1, WAVES), 2.0 / LONS)
    scale[0, 0, 0] = 1.0 / LONS
    scale[0, 0, WAVES // 2] = 0.0

    def halves(x):
        x = x.astype(np.float32)
        hi = x.astype(jnp.bfloat16)
        return np.stack([hi, (x - hi.astype(np.float32)).astype(jnp.bfloat16)], axis=1)

    return halves(back * scale)


ANY = pl.BlockSpec(memory_space=pl.ANY)
VM = pl.BlockSpec(memory_space=pltpu.VMEM)
DMA = pltpu.SemaphoreType.DMA
LIMIT = 35 * 1024 * 1024
LIMIT_END = 18 * 1024 * 1024


def solution(mesh):
    table = dft_tables()

    def per_device(coef, legendre, gauss_weight):
        _, spec_mid, last, leg_last, grid_mid = pl.pallas_call(
            transform,
            out_shape=(
                jax.ShapeDtypeStruct((KK, 2, WAVES, LANES), F32),
                pltpu.VMEM((EARLY_WAVES, 2, LEVS, WAVES), F32),
                pltpu.VMEM((DEVS, KK, 2, CHUNK, LANES), F32),
                pltpu.VMEM((NB, 2, WAVES, LANES), F32),
                pltpu.VMEM((LEVS, LAT, LONS), F32),
            ),
            in_specs=[ANY, ANY, ANY, ANY],
            out_specs=(ANY, VM, VM, VM, VM),
            scratch_shapes=[
                pltpu.VMEM((2, 2, HALF, WAVES), BF),
                pltpu.VMEM((2, 2, WAVES, HALF), BF),
                pltpu.VMEM((LATS,), F32),
                pltpu.VMEM((NB, 2, LEVS, WAVES), F32),
                pltpu.VMEM((2, WAVES, LANES), F32),
                pltpu.VMEM((KK, 2, WAVES, LANES), F32),
                pltpu.VMEM((DEVS, 2, KK, 2, OWN // 2, LANES), F32),
                DMA((NB,)), DMA((2 * NB,)), DMA((NB, 2)), DMA,
                DMA((DEVS,)), DMA((DEVS,)), DMA((KK, DEVS)), DMA((KK, DEVS)), DMA((DEVS,)), DMA((DEVS,)), DMA((CHUNKS, DEVS)), DMA((2,)),
            ],
            compiler_params=pltpu.CompilerParams(collective_id=0, has_side_effects=True, vmem_limit_bytes=LIMIT),
            name='transform',
        )(coef, legendre, table, gauss_weight)
        grid, spec_out = pl.pallas_call(
            finish,
            out_shape=(jax.ShapeDtypeStruct((LEVS, LAT, LONS), F32), jax.ShapeDtypeStruct((OWN, 2, LEVS, WAVES), F32)),
            in_specs=[VM, VM, ANY, ANY, ANY],
            out_specs=(ANY, ANY),
            scratch_shapes=[
                pltpu.VMEM((CHUNK - NB, WAVES, LATS), F32),
                pltpu.VMEM((CHUNK, 2, LEVS, WAVES), F32),
                DMA((CHUNK - NB,)), DMA((CHUNK,)), DMA((CHUNK,)), DMA((EARLY_WAVES,)),
            ],
            compiler_params=pltpu.CompilerParams(vmem_limit_bytes=LIMIT_END),
            name='finish',
        )(last, leg_last, legendre, grid_mid, spec_mid)
        return grid, spec_out

    return jax.shard_map(per_device, mesh=mesh, in_specs=(P('w', None, 'lev', None), P(None, None, None), P(None)), out_specs=(P('lev', 'w', None), P('w', None, 'lev', None)), check_vma=False)
```

```python
import functools

import jax
import jax.numpy as jnp
import numpy as np
from jax import lax
from jax.experimental import pallas as pl
from jax.experimental.pallas import tpu as pltpu
from jax.sharding import PartitionSpec as P

DEVS = 8
WAVES = 512
OWN = WAVES // DEVS
LATS = 768
LAT = LATS // DEVS
LEVS = 32
LONS = 1024
HALF = LONS // 2
KK = 8
QQ = 4
ORDER = (6, 5, 7, 4, 2, 3, 1, 0)
SIDE = 4
LANES = QQ * LAT
CHUNK = 8
NB = 6
CHUNKS = OWN // CHUNK
FIRST = 6
EARLY = 2
AHEAD = 6
EARLY_WAVES = OWN - CHUNK
BF = jnp.bfloat16
F32 = jnp.float32


def split(x):
    hi = x.astype(BF)
    return hi, (x - hi.astype(F32)).astype(BF)


def dot3(a_hi, a_lo, b_hi, b_lo, dims):
    mm = functools.partial(lax.dot_general, dimension_numbers=(dims, ((), ())), preferred_element_type=F32)
    return mm(a_hi, b_hi) + (mm(a_hi, b_lo) + mm(a_lo, b_hi))


def dot_stacked(a, b, dims):
    rows = a.shape[0]
    (a_hi, a_lo), (b_hi, b_lo) = split(a), split(b)
    mm = functools.partial(lax.dot_general, dimension_numbers=(dims, ((), ())), preferred_element_type=F32)
    both = mm(jnp.concatenate([a_hi, a_lo], axis=0), b_hi)
    return both[:rows] + (both[rows:] + mm(a_hi, b_lo))


def barrier_signal(me):
    sem = pltpu.get_barrier_semaphore()
    for o in range(1, DEVS):
        pl.semaphore_signal(sem, inc=1, device_id={'w': lax.rem(me + o, DEVS)}, device_id_type=pl.DeviceIdType.MESH)


def barrier_wait():
    pl.semaphore_wait(pltpu.get_barrier_semaphore(), DEVS - 1)


def own_wave(t):
    return 2 * lax.rem(t, OWN // 2) + lax.div(t, OWN // 2)


def gather_rows(hbuf, i):
    rows = []
    for r in range(2):
        parts = [jnp.concatenate([hbuf[d, kk, r, pl.ds(i, 1), :] for kk in range(KK)], axis=0) for d in range(DEVS)]
        for q in range(QQ):
            rows.append(jnp.concatenate([p[:, q * LAT:(q + 1) * LAT] for p in parts], axis=1))
    return jnp.concatenate(rows, axis=0)


def whole(lbuf, slot):
    return jnp.concatenate([lbuf[slot, 0], lbuf[slot, 1]], axis=1)


def transform(coef, leg, table, weight_in, frecv, spec_out, last_out, lbuf, grid_out, dft, dft_t, weight, cbuf, fbuf, both, hrecv, csem, hsem, lsem, fsem, fs1, fr1, fs2, fr2, ssem, asem, bsem, tsem):
    me = lax.axis_index('w')
    barrier_signal(me)

    row, col = lax.div(me, SIDE), lax.rem(me, SIDE)

    def fetch_half(u):
        t = lax.div(u, 2 * CHUNK) * CHUNK + lax.rem(u, CHUNK)
        side = lax.rem(row + 1 + lax.rem(lax.div(u, CHUNK), 2), 2)
        cols = pl.ds(pl.multiple_of(side * LANES, LANES), LANES)
        buf = lax.rem(u, 2 * NB)
        return pltpu.make_async_copy(leg.at[me * OWN + own_wave(t), :, cols], lbuf.at[lax.div(buf, 2), lax.rem(buf, 2)], hsem.at[buf])

    def fetch_coef(u):
        t = lax.div(u, 2 * CHUNK) * CHUNK + lax.rem(u, CHUNK)
        slot = lax.rem(u, NB)
        return pltpu.make_async_copy(coef.at[own_wave(t)], cbuf.at[slot], csem.at[slot])

    def fetch_leg(t, half):
        slot = lax.rem(t, NB)
        cols = pl.ds(half * LANES, LANES)
        return pltpu.make_async_copy(leg.at[me * OWN + own_wave(t), :, cols], lbuf.at[slot, half], lsem.at[slot, half])

    def row_of(o):
        return row if o < SIDE else 1 - row

    def target(o):
        return row_of(o) * SIDE + lax.rem(col + o, SIDE)

    def source(o):
        return row_of(o) * SIDE + lax.rem(col - o + DEVS, SIDE)

    def block(d, row=0, size=OWN):
        return pl.ds(pl.multiple_of(d * OWN + row, CHUNK), size)

    def move(o, src_ref, dst_ref, send_sem, recv_sem):
        if o == 0:
            pltpu.make_async_copy(src_ref, dst_ref, recv_sem).start()
        else:
            pltpu.make_async_remote_copy(src_ref=src_ref, dst_ref=dst_ref, send_sem=send_sem, recv_sem=recv_sem, device_id={'w': target(o)}, device_id_type=pl.DeviceIdType.MESH).start()

    def wait_for(part, sem):
        pltpu.make_async_copy(part, part, sem).wait()

    for u in range(NB):
        fetch_coef(u).start()
    for u in range(2 * NB):
        fetch_half(u).start()
    constants = (pltpu.make_async_copy(table, dft, tsem.at[0]), pltpu.make_async_copy(weight_in, weight, tsem.at[1]))
    for copy in constants:
        copy.start()

    @pl.loop(0, CHUNKS)
    def _(c):
        for part in range(2):
            side = lax.rem(row + 1 + part, 2)

            @pl.loop(0, CHUNK)
            def _(i):
                u = (2 * c + part) * CHUNK + i
                t = c * CHUNK + i
                fetch_half(u).wait()
                fetch_coef(u).wait()
                buf = lax.rem(u, 2 * NB)
                f = dot_stacked(cbuf[lax.rem(u, NB)].reshape(2 * LEVS, WAVES), lbuf[lax.div(buf, 2), lax.rem(buf, 2)], ((1,), (0,)))

                @pl.when(u + 2 * NB < 2 * OWN)
                def _():
                    fetch_half(u + 2 * NB).start()

                @pl.when(u + NB < 2 * OWN)
                def _():
                    fetch_coef(u + NB).start()

                for j in range(SIDE):
                    cols = f[:, j * LAT:(j + 1) * LAT]
                    for r in range(2):
                        packed = jnp.concatenate([cols[r * LEVS + q * KK:r * LEVS + (q + 1) * KK] for q in range(QQ)], axis=1)
                        for kk in range(KK):
                            both[kk, r, pl.ds((side * SIDE + j) * OWN + t, 1), :] = packed[kk:kk + 1]

            if part == 0:
                @pl.when(c == 0)
                def _():
                    barrier_wait()

            for o in ORDER[part * SIDE:(part + 1) * SIDE]:
                move(o, both.at[pl.ds(0, FIRST), :, block(target(o), c * CHUNK, CHUNK), :], frecv.at[pl.ds(0, FIRST), :, block(me, c * CHUNK, CHUNK), :], fs1.at[o], fr1.at[o])

    for kk in range(FIRST, KK):
        for o in ORDER:
            move(o, both.at[kk, :, block(target(o)), :], frecv.at[kk, :, block(me), :], fs2.at[kk, o], fr2.at[kk, o])
    for t in range(NB):
        for half in range(2):
            fetch_leg(t, half).start()

    for copy in constants:
        copy.wait()
    weights = weight[...].reshape(1, LATS)
    own_weight = weights[:, 0:LAT]
    for d in range(1, DEVS):
        own_weight = jnp.where(me == d, weights[:, d * LAT:(d + 1) * LAT], own_weight)
    own_weight = jnp.concatenate([own_weight] * QQ, axis=1)
    rows = lax.broadcasted_iota(jnp.int32, (WAVES, 1), 0)
    for par in range(2):
        unscale = jnp.where(rows == 0, 1.0 * LONS, 1.0 * HALF) if par == 0 else 1.0 * HALF
        for half in range(2):
            dft_t[par, half] = (dft[par, half].astype(F32).T * unscale).astype(BF)

    def dst_rows(o, row, size):
        return pl.ds(pl.multiple_of(target(o) * (OWN // 2) + row, CHUNK), size)

    def send_levels(kk):
        for o in ORDER:
            for par in range(2):
                move(o, both.at[kk, :, dst_rows(o, par * (WAVES // 2), OWN // 2), :], hrecv.at[me, par, kk], ssem.at[o], asem.at[o])

    def chunk_at(ref, c):
        row = pl.multiple_of(lax.rem(c, 4) * CHUNK, CHUNK)
        return ref.at[lax.div(c, 4), pl.ds(EARLY, KK - EARLY), :, pl.ds(row, CHUNK), :]

    def send_chunk(c):
        row = lax.div(c, 4) * (WAVES // 2) + lax.rem(c, 4) * CHUNK
        for o in ORDER:
            move(o, both.at[pl.ds(EARLY, KK - EARLY), :, dst_rows(o, row, CHUNK), :], chunk_at(hrecv.at[me], c), ssem.at[o], bsem.at[c, o])

    def arrived(c):
        for o in range(DEVS):
            wait_for(chunk_at(hrecv.at[source(o)], c), bsem.at[c, o])

    @pl.loop(0, KK)
    def _(kk):
        @pl.when(kk == 0)
        def _():
            for o in range(DEVS):
                wait_for(frecv.at[pl.ds(0, FIRST), :, block(source(o)), :], fr1.at[o])
            for o in range(1, DEVS):
                wait_for(both.at[pl.ds(0, FIRST), :, block(target(o)), :], fs1.at[o])

        @pl.when(kk >= FIRST)
        def _():
            for o in range(DEVS):
                wait_for(frecv.at[kk, :, block(source(o)), :], fr2.at[kk, o])
            for o in range(1, DEVS):
                wait_for(both.at[kk, :, block(target(o)), :], fs2.at[kk, o])

        fetch = pltpu.make_async_copy(frecv.at[kk], fbuf, fsem)
        fetch.start()
        fetch.wait()

        sums = []
        for par in range(2):
            x = jnp.concatenate([fbuf[r, d * OWN + par * (OWN // 2):d * OWN + (par + 1) * (OWN // 2), :] for r in range(2) for d in range(DEVS)], axis=0)
            x_hi, x_lo = split(x)
            sums.append(dot3(dft[par, 0], dft[par, 1], x_hi, x_lo, ((1,), (0,))))
        first, second = sums[0] + sums[1], sums[0] - sums[1]
        for half, y in enumerate((first.T, second.T)):
            for q in range(QQ):
                grid_out[q * KK + kk, :, half * HALF:(half + 1) * HALF] = y[q * LAT:(q + 1) * LAT]
        first, second = first * first, second * second
        for par, y in enumerate((first + second, first - second)):
            y_hi, y_lo = split(y)
            h = dot3(dft_t[par, 0], dft_t[par, 1], y_hi, y_lo, ((1,), (0,))) * own_weight
            for r in range(2):
                both[kk, r, par * (WAVES // 2):(par + 1) * (WAVES // 2), :] = h[r * (WAVES // 2):(r + 1) * (WAVES // 2)]

        @pl.when(kk < EARLY)
        def _():
            send_levels(kk)

    for c in range(AHEAD):
        send_chunk(c)
    for o in range(DEVS):
        wait_for(hrecv.at[source(o), :, pl.ds(0, EARLY)], asem.at[o])

    @pl.loop(0, CHUNKS - 1)
    def _(c):
        arrived(c)

        @pl.when(c + AHEAD < CHUNKS)
        def _():
            send_chunk(c + AHEAD)

        par, row = lax.div(c, 4), lax.rem(c, 4) * CHUNK

        @pl.loop(0, CHUNK)
        def _(i):
            t = c * CHUNK + i
            h = gather_rows(hrecv.at[:, par], row + i)
            for half in range(2):
                fetch_leg(t, half).wait()
            spec_out[t] = dot_stacked(h, whole(lbuf, lax.rem(t, NB)), ((1,), (1,))).reshape(2, LEVS, WAVES)

            @pl.when(t + NB < OWN)
            def _():
                for half in range(2):
                    fetch_leg(t + NB, half).start()

    for t in range(EARLY_WAVES, EARLY_WAVES + NB):
        for half in range(2):
            fetch_leg(t, half).wait()
    for o in (0, 6, 5, 7, 4, 2, 3, 1):
        d = source(o)
        wait_for(chunk_at(hrecv.at[d], CHUNKS - 1), bsem.at[CHUNKS - 1, o])
        last_out[d] = hrecv[d, 1, :, :, 3 * CHUNK:4 * CHUNK, :]
    for o in range(1, DEVS):
        wait_for(both.at[:, :, block(target(o)), :], ssem.at[o])


def finish(h_in, leg_in, leg, grid_in, spec_in, grid_out, spec_out, lbuf, obuf, lsem, osem, gsem, ssem):
    me = lax.axis_index('w')

    def fetch_leg(i):
        return pltpu.make_async_copy(leg.at[me * OWN + own_wave(EARLY_WAVES + i)], lbuf.at[i - NB], lsem.at[i - NB])

    def grid_copy(i):
        return pltpu.make_async_copy(grid_in.at[pl.ds(i * QQ, QQ)], grid_out.at[pl.ds(i * QQ, QQ)], gsem.at[i])

    def spec_copy(t):
        return pltpu.make_async_copy(spec_in.at[t], spec_out.at[own_wave(t)], ssem.at[t])

    def store(i):
        return pltpu.make_async_copy(obuf.at[i], spec_out.at[own_wave(EARLY_WAVES + i)], osem.at[i])

    for i in range(NB, CHUNK):
        fetch_leg(i).start()
    for i in range(CHUNK):
        grid_copy(i).start()

    @pl.loop(0, EARLY_WAVES)
    def _(t):
        spec_copy(t).start()

    @pl.loop(0, NB)
    def _(i):
        block = whole(leg_in, lax.rem(EARLY_WAVES + i, NB))
        obuf[i] = dot_stacked(gather_rows(h_in, i), block, ((1,), (1,))).reshape(2, LEVS, WAVES)
        store(i).start()

    @pl.loop(NB, CHUNK)
    def _(i):
        h = gather_rows(h_in, i)
        fetch_leg(i).wait()
        obuf[i] = dot_stacked(h, lbuf[i - NB], ((1,), (1,))).reshape(2, LEVS, WAVES)
        store(i).start()

    @pl.loop(0, CHUNK)
    def _(i):
        store(i).wait()
        grid_copy(i).wait()

    @pl.loop(0, EARLY_WAVES)
    def _(t):
        spec_copy(t).wait()


def dft_tables():
    n = np.arange(HALF)[:, None]
    tabs = []
    for par in range(2):
        m = np.arange(par, WAVES, 2)[None, :]
        ang = 2 * np.pi * ((m * n) % LONS) / LONS
        tabs.append(np.concatenate([np.cos(ang), -np.sin(ang)], axis=1))
    back = np.stack(tabs)
    scale = np.full((2, 1, WAVES), 2.0 / LONS)
    scale[0, 0, 0] = 1.0 / LONS
    scale[0, 0, WAVES // 2] = 0.0

    def halves(x):
        x = x.astype(np.float32)
        hi = x.astype(jnp.bfloat16)
        return np.stack([hi, (x - hi.astype(np.float32)).astype(jnp.bfloat16)], axis=1)

    return halves(back * scale)


ANY = pl.BlockSpec(memory_space=pl.ANY)
VM = pl.BlockSpec(memory_space=pltpu.VMEM)
DMA = pltpu.SemaphoreType.DMA
LIMIT = 35100 * 1024
LIMIT_END = 18 * 1024 * 1024


def solution(mesh):
    table = dft_tables()

    def per_device(coef, legendre, gauss_weight):
        _, spec_mid, last, leg_last, grid_mid = pl.pallas_call(
            transform,
            out_shape=(
                jax.ShapeDtypeStruct((KK, 2, WAVES, LANES), F32),
                pltpu.VMEM((EARLY_WAVES, 2, LEVS, WAVES), F32),
                pltpu.VMEM((DEVS, KK, 2, CHUNK, LANES), F32),
                pltpu.VMEM((NB, 2, WAVES, LANES), F32),
                pltpu.VMEM((LEVS, LAT, LONS), F32),
            ),
            in_specs=[ANY, ANY, ANY, ANY],
            out_specs=(ANY, VM, VM, VM, VM),
            scratch_shapes=[
                pltpu.VMEM((2, 2, HALF, WAVES), BF),
                pltpu.VMEM((2, 2, WAVES, HALF), BF),
                pltpu.VMEM((LATS,), F32),
                pltpu.VMEM((NB, 2, LEVS, WAVES), F32),
                pltpu.VMEM((2, WAVES, LANES), F32),
                pltpu.VMEM((KK, 2, WAVES, LANES), F32),
                pltpu.VMEM((DEVS, 2, KK, 2, OWN // 2, LANES), F32),
                DMA((NB,)), DMA((2 * NB,)), DMA((NB, 2)), DMA,
                DMA((DEVS,)), DMA((DEVS,)), DMA((KK, DEVS)), DMA((KK, DEVS)), DMA((DEVS,)), DMA((DEVS,)), DMA((CHUNKS, DEVS)), DMA((2,)),
            ],
            compiler_params=pltpu.CompilerParams(collective_id=0, has_side_effects=True, vmem_limit_bytes=LIMIT),
            name='transform',
        )(coef, legendre, table, gauss_weight)
        grid, spec_out = pl.pallas_call(
            finish,
            out_shape=(jax.ShapeDtypeStruct((LEVS, LAT, LONS), F32), jax.ShapeDtypeStruct((OWN, 2, LEVS, WAVES), F32)),
            in_specs=[VM, VM, ANY, ANY, ANY],
            out_specs=(ANY, ANY),
            scratch_shapes=[
                pltpu.VMEM((CHUNK - NB, WAVES, LATS), F32),
                pltpu.VMEM((CHUNK, 2, LEVS, WAVES), F32),
                DMA((CHUNK - NB,)), DMA((CHUNK,)), DMA((CHUNK,)), DMA((EARLY_WAVES,)),
            ],
            compiler_params=pltpu.CompilerParams(vmem_limit_bytes=LIMIT_END),
            name='finish',
        )(last, leg_last, legendre, grid_mid, spec_mid)
        return grid, spec_out

    return jax.shard_map(per_device, mesh=mesh, in_specs=(P('w', None, 'lev', None), P(None, None, None), P(None)), out_specs=(P('lev', 'w', None), P('w', None, 'lev', None)), check_vma=False)
```
